32 devices in a mesh: shard: 8 (over y, x, core), head: 4 (over z).
Axes of the slice: x: 2, y: 2, z: 4, core: 2. Of those that a mesh axis runs over, the one named last changes fastest.
Arguments:
- block_in: bfloat16 [4, 4096, 768], P(None, ('shard', 'head')), may hold values from -6 to 6
- gain_in: float32 [768], replicated, may hold values from 0.5 to 1.5
- w_in: bfloat16 [768, 3352], P(('shard', 'head')), may hold values from -0.21875 to 0.21875
- conv_w: float32 [4, 1792], replicated, may hold values from -3 to 3
- conv_b: float32 [1792], replicated, may hold values from -3 to 3
- dt_bias: float32 [24], replicated, may hold values from -4.5 to 1
- a_log: float32 [24], replicated, may hold values from -12 to 0
- d_skip: float32 [24], replicated, may hold values from 0.5 to 1.5
- gain_out: float32 [1536], replicated, may hold values from 0.5 to 1.5
- w_out: bfloat16 [1536, 768], P(('shard', 'head')), may hold values from -0.15625 to 0.15625
- out_grad: bfloat16 [4, 4096, 768], P(None, ('shard', 'head')), may hold values from -6 to 6
Outputs:
- block_out: bfloat16 [4, 4096, 768], P(None, ('shard', 'head'))
- in_grad: float32 [4, 4096, 768], P(None, ('shard', 'head'))
- gain_in_grad: float32 [768], replicated
- w_in_grad: float32 [768, 3352], P(('shard', 'head'))
- conv_w_grad: float32 [4, 1792], replicated
- conv_b_grad: float32 [1792], replicated
- dt_bias_grad: float32 [24], replicated
- a_log_grad: float32 [24], replicated
- d_skip_grad: float32 [24], replicated
- gain_out_grad: float32 [1536], replicated
- w_out_grad: float32 [1536, 768], P(('shard', 'head'))
The draws below stay inside these ranges and needn't reach their ends.
All inputs are finite; a program needn't handle non-finite values.
Results may differ from the reference program's by a relative error of at most 0.011.
Values may be sent and summed in bfloat16 or wider, within the bound.
A program may use at most 192 MiB of HBM per device.

```python
import jax
import jax.numpy as jnp
from jax import lax

D = 768
HEADS = 24
CONV = 4
BLOCK = 256
SEQS = 4
INNER = 1536
CONV_CH = 1792
PROJ = 3352
LENGTH = 4096
N_HEAD = 4


def slow_heads(key):
    picks = jax.random.uniform(jax.random.fold_in(key, 101), (HEADS,), jnp.float32)
    share = 0.5
    return picks < share


def head_biases(key):
    offsets = jax.random.uniform(jax.random.fold_in(key, 202), (HEADS,), jnp.float32)
    return jnp.where(slow_heads(key), offsets - 4.5, offsets)


def draw_dt_bias(key, part):
    return head_biases(key)


def draw_a_log(key, part):
    spread = jax.random.uniform(jax.random.fold_in(key, 303), (HEADS,), jnp.float32)
    slow_low = jnp.log(0.2 / LENGTH)
    slow_high = jnp.log(1.2 / LENGTH)
    fast_low = jnp.log(0.02)
    fast_high = jnp.log(0.05)
    log_rates = jnp.where(slow_heads(key), slow_low + spread * (slow_high - slow_low), fast_low + spread * (fast_high - fast_low))
    return log_rates - jnp.log(jax.nn.softplus(head_biases(key)))


def block_levels(stream_key, extent, pieces, low, high):
    level, own = 1.0, jax.random.fold_in(stream_key, 6)
    for dim, parts in pieces:
        draws = jnp.exp(jax.random.uniform(jax.random.fold_in(own, dim), (parts,), jnp.float32, low / len(pieces), high / len(pieces)))
        level = level * jnp.repeat(draws, extent[dim] // parts).reshape([-1 if axis == dim else 1 for axis in range(len(extent))])
    return level


def gaussian(own_key, dims, scale, most, cuts=(), held_as=jnp.bfloat16):
    array = jax.random.normal(own_key, dims, jnp.float32) * scale
    if len(cuts) > 0:
        array = block_levels(own_key, dims, cuts, -0.22, 0.18) * array
    return jnp.clip(array, min=-most, max=most).astype(held_as)


def setup_inputs(seed: int = 0) -> dict:
    key_list = jax.random.split(jax.random.key(seed), 12)
    block_in = gaussian(key_list[0], (SEQS, LENGTH, D), 1.0, 6.0, ((1, 32),))
    gain_in = jnp.clip(1.0 + 0.1 * jax.random.normal(key_list[1], (D,), jnp.float32), 0.5, 1.5)
    w_in = gaussian(key_list[2], (D, PROJ), D ** -0.5, 0.21875, ((0, 32),))
    conv_w = gaussian(key_list[3], (CONV, CONV_CH), CONV ** -0.5, 3.0, (), jnp.float32)
    conv_b = gaussian(key_list[4], (CONV_CH,), 0.5, 3.0, (), jnp.float32)
    dt_bias = draw_dt_bias(jax.random.fold_in(key_list[11], 71), 0)
    a_log = draw_a_log(jax.random.fold_in(key_list[11], 71), 0)
    d_skip = jnp.clip(jax.random.uniform(key_list[7], (HEADS,), jnp.float32, 0.5, 1.5), 0.5, 1.5)
    gain_out = jnp.clip(1.0 + 0.1 * jax.random.normal(key_list[8], (INNER,), jnp.float32), 0.5, 1.5)
    w_out = gaussian(key_list[9], (INNER, D), INNER ** -0.5, 0.15625, ((0, 32),))
    out_grad = gaussian(key_list[10], (SEQS, LENGTH, D), 1.0, 6.0, ((1, 32),))
    return {"block_in": block_in, "gain_in": gain_in, "w_in": w_in, "conv_w": conv_w, "conv_b": conv_b, "dt_bias": dt_bias, "a_log": a_log, "d_skip": d_skip, "gain_out": gain_out, "w_out": w_out, "out_grad": out_grad}


EPSILON = 1e-05
HIGHEST = lax.Precision.HIGHEST

def silu_slope(values):
    logistic = jax.nn.sigmoid(values)
    return logistic * (1.0 + values * (1.0 - logistic))

def block_scan(x_heads, b_rows, c_rows, step_rates, deltas, initial, block_size):
    length, head_count, head_dim = x_heads.shape
    block_count = length // block_size
    causal = jnp.arange(block_size)[:, None] >= jnp.arange(block_size)[None, :]

    def advance(carried, sliced):
        x_block, b_block, c_block, delta_block, rate_block = sliced
        running = jnp.cumsum(rate_block, axis=0)
        spread = running[:, None, :] - running[None, :, :]
        decay_matrix = jnp.exp(jnp.where(causal[:, :, None], spread, -jnp.inf))
        scores = jnp.dot(c_block, b_block.T, precision=HIGHEST)
        mixing = scores[:, :, None] * decay_matrix * delta_block[None, :, :]
        inside = jnp.einsum('tsh,shp->thp', mixing, x_block, precision=HIGHEST)
        from_state = jnp.einsum('tn,hpn->thp', c_block, carried, precision=HIGHEST) * jnp.exp(running)[:, :, None]
        last_rate = running[-1]
        tail_weights = jnp.exp(last_rate[None, :] - running) * delta_block
        updated = carried * jnp.exp(last_rate)[:, None, None] + jnp.einsum('sh,shp,sn->hpn', tail_weights, x_block, b_block, precision=HIGHEST)
        return (updated, inside + from_state)
    blocks = (x_heads.reshape(block_count, block_size, head_count, head_dim), b_rows.reshape(block_count, block_size, -1), c_rows.reshape(block_count, block_size, -1), deltas.reshape(block_count, block_size, head_count), step_rates.reshape(block_count, block_size, head_count))
    final_state, outputs = lax.scan(advance, initial, blocks)
    return (outputs.reshape(length, head_count, head_dim), final_state)

def causal_conv(padded, taps_weight, bias, length):
    summed = jnp.zeros((length, padded.shape[1]), jnp.float32) + bias[None, :]
    for offset in range(taps_weight.shape[0]):
        summed = summed + taps_weight[offset][None, :] * padded[offset:offset + length]
    return summed

def mixer_local(padded_x, padded_bc, dt_in, weight_x, bias_x, weight_bc, bias_bc, bias_dt, log_rate, skip_gain, initial, block_size):
    length, head_count = dt_in.shape
    x_act = jax.nn.silu(causal_conv(padded_x, weight_x, bias_x, length))
    bc_act = jax.nn.silu(causal_conv(padded_bc, weight_bc, bias_bc, length))
    state_size = bc_act.shape[1] // 2
    b_rows = bc_act[:, :state_size]
    c_rows = bc_act[:, state_size:]
    deltas = jax.nn.softplus(dt_in + bias_dt[None, :])
    step_rates = deltas * (-jnp.exp(log_rate))[None, :]
    x_heads = x_act.reshape(length, head_count, -1)
    outputs, final_state = block_scan(x_heads, b_rows, c_rows, step_rates, deltas, initial, block_size)
    outputs = outputs + skip_gain[None, :, None] * x_heads
    return (outputs, final_state, jnp.cumsum(step_rates, axis=0), c_rows)

def reference(block_in, gain_in, w_in, conv_w, conv_b, dt_bias, a_log, d_skip, gain_out, w_out, out_grad):
    inner_width = gain_out.shape[0]
    head_count = dt_bias.shape[0]
    state_size = (conv_b.shape[0] - inner_width) // 2
    conv_taps = conv_w.shape[0]
    margin = conv_taps - 1
    length = block_in.shape[1]
    head_dim = inner_width // head_count
    groups = N_HEAD
    heads_group = head_count // groups
    inner_group = inner_width // groups
    initial = jnp.zeros((heads_group, head_dim, state_size), jnp.float32)

    def run_group(padded_x, padded_bc, dt_in, weight_x, bias_x, weight_bc, bias_bc, bias_dt, log_rate, skip_gain):
        outputs = mixer_local(padded_x, padded_bc, dt_in, weight_x, bias_x, weight_bc, bias_bc, bias_dt, log_rate, skip_gain, initial, BLOCK)
        return outputs[0]
    run_groups = jax.vmap(run_group)
    group_wx = conv_w[:, :inner_width].reshape(conv_taps, groups, inner_group).transpose(1, 0, 2)
    group_bx = conv_b[:inner_width].reshape(groups, inner_group)
    group_wbc = jnp.broadcast_to(conv_w[:, inner_width:][None], (groups, conv_taps, 2 * state_size))
    group_bbc = jnp.broadcast_to(conv_b[inner_width:][None], (groups, 2 * state_size))
    group_bdt = dt_bias.reshape(groups, heads_group)
    group_alog = a_log.reshape(groups, heads_group)
    group_skip = d_skip.reshape(groups, heads_group)

    def per_sequence(totals, sliced):
        tokens, cotangent = sliced
        tokens_f = tokens.astype(jnp.float32)
        rms_in = lax.rsqrt(lax.optimization_barrier(jnp.mean(tokens_f * tokens_f, axis=-1, keepdims=True)) + EPSILON)
        normed = (tokens_f * rms_in * gain_in[None, :]).astype(jnp.bfloat16)
        projected = jnp.dot(normed, w_in, preferred_element_type=jnp.float32)
        gate_in = projected[:, :inner_width].astype(jnp.bfloat16)
        x_raw = projected[:, inner_width:2 * inner_width].astype(jnp.bfloat16)
        bc_raw = projected[:, 2 * inner_width:2 * inner_width + 2 * state_size].astype(jnp.bfloat16)
        dt_raw = projected[:, 2 * inner_width + 2 * state_size:].astype(jnp.bfloat16)
        padded_x = jnp.concatenate([jnp.zeros((margin, inner_width), jnp.float32), x_raw.astype(jnp.float32)], axis=0)
        padded_bc = jnp.concatenate([jnp.zeros((margin, 2 * state_size), jnp.float32), bc_raw.astype(jnp.float32)], axis=0)
        group_px = padded_x.reshape(length + margin, groups, inner_group).transpose(1, 0, 2)
        group_pbc = jnp.broadcast_to(padded_bc[None], (groups, length + margin, 2 * state_size))
        group_dt = dt_raw.astype(jnp.float32).reshape(length, groups, heads_group).transpose(1, 0, 2)
        mixed_groups, pullback = jax.vjp(run_groups, group_px, group_pbc, group_dt, group_wx, group_bx, group_wbc, group_bbc, group_bdt, group_alog, group_skip)
        mixed_b = mixed_groups.transpose(1, 0, 2, 3).reshape(length, inner_width).astype(jnp.bfloat16)
        mixed_f = mixed_b.astype(jnp.float32)
        gate_f = gate_in.astype(jnp.float32)
        gated_out = mixed_f * jax.nn.silu(gate_f)
        rms_out = lax.rsqrt(lax.optimization_barrier(jnp.mean(gated_out * gated_out, axis=-1, keepdims=True)) + EPSILON)
        gnormed = (gated_out * rms_out * gain_out[None, :]).astype(jnp.bfloat16)
        result = (tokens_f + jnp.dot(gnormed, w_out, preferred_element_type=jnp.float32)).astype(jnp.bfloat16)
        grad_gnormed = jnp.dot(cotangent, w_out.T, preferred_element_type=jnp.float32)
        grad_w_out = jnp.dot(gnormed.T, cotangent, preferred_element_type=jnp.float32)
        grad_gain_out = lax.optimization_barrier(jnp.sum(grad_gnormed * gated_out * rms_out, axis=0))
        scaled_out = grad_gnormed * gain_out[None, :]
        grad_gated = rms_out * scaled_out - gated_out * rms_out ** 3 * lax.optimization_barrier(jnp.mean(gated_out * scaled_out, axis=-1, keepdims=True))
        grad_mixed = (grad_gated * jax.nn.silu(gate_f)).astype(jnp.bfloat16)
        grad_gate = grad_gated * mixed_f * silu_slope(gate_f)
        cot_groups = grad_mixed.astype(jnp.float32).reshape(length, groups, heads_group, head_dim).transpose(1, 0, 2, 3)
        pulled = pullback(cot_groups)
        grad_px = pulled[0].transpose(1, 0, 2).reshape(length + margin, inner_width)
        bc_parts = lax.optimization_barrier(pulled[1].astype(jnp.bfloat16))
        grad_pbc = lax.optimization_barrier(jnp.sum(bc_parts.astype(jnp.float32), axis=0))
        grad_dt = pulled[2].transpose(1, 0, 2).reshape(length, head_count)
        grad_proj = jnp.concatenate([grad_gate.astype(jnp.bfloat16), grad_px[margin:].astype(jnp.bfloat16), grad_pbc[margin:].astype(jnp.bfloat16), grad_dt.astype(jnp.bfloat16)], axis=1)
        grad_w_in = jnp.dot(normed.T, grad_proj, preferred_element_type=jnp.float32)
        grad_normed = jnp.dot(grad_proj, w_in.T, preferred_element_type=jnp.float32)
        grad_gain_in = lax.optimization_barrier(jnp.sum(grad_normed * tokens_f * rms_in, axis=0))
        scaled_in = grad_normed * gain_in[None, :]
        grad_tokens = cotangent.astype(jnp.float32) + rms_in * scaled_in - tokens_f * rms_in ** 3 * lax.optimization_barrier(jnp.mean(tokens_f * scaled_in, axis=-1, keepdims=True))
        grad_wx = pulled[3].transpose(1, 0, 2).reshape(conv_taps, inner_width)
        grad_bx = pulled[4].reshape(inner_width)
        grad_conv_w = jnp.concatenate([grad_wx, lax.optimization_barrier(jnp.sum(pulled[5], axis=0))], axis=1)
        grad_conv_b = jnp.concatenate([grad_bx, lax.optimization_barrier(jnp.sum(pulled[6], axis=0))], axis=0)
        updates = (grad_gain_in, grad_w_in, grad_conv_w, grad_conv_b, pulled[7].reshape(head_count), pulled[8].reshape(head_count), pulled[9].reshape(head_count), grad_gain_out, grad_w_out)
        totals = jax.tree.map(lambda first_term, second_term: first_term + second_term, totals, updates)
        return (totals, (result, grad_tokens))
    zeros_init = (jnp.zeros(gain_in.shape, jnp.float32), jnp.zeros(w_in.shape, jnp.float32), jnp.zeros(conv_w.shape, jnp.float32), jnp.zeros(conv_b.shape, jnp.float32), jnp.zeros(dt_bias.shape, jnp.float32), jnp.zeros(a_log.shape, jnp.float32), jnp.zeros(d_skip.shape, jnp.float32), jnp.zeros(gain_out.shape, jnp.float32), jnp.zeros(w_out.shape, jnp.float32))
    totals, emitted = lax.scan(per_sequence, zeros_init, (block_in, out_grad))
    block_out, in_grad = emitted
    return (block_out, in_grad, totals[0], totals[1], totals[2], totals[3], totals[4], totals[5], totals[6], totals[7], totals[8])
```

```python
import functools

import jax
import jax.numpy as jnp
from jax import lax
from jax.experimental import pallas as pl
from jax.experimental.pallas import tpu as pltpu
from jax.sharding import PartitionSpec as P

F32, BF16 = jnp.float32, jnp.bfloat16
EPSILON = 1e-05
HIGHEST = lax.Precision.HIGHEST
CHUNK = 128
HALO = 16
LANES = 128
VMEM_LIMIT = 60 * 1024 * 1024


def dot(a, b, contract=((1,), (0,)), precision=None):
    return lax.dot_general(a, b, (contract, ((), ())), precision=precision, preferred_element_type=F32)


ROWS = ((0,), (0,))
LAST = ((1,), (1,))


def tile_of(rows, most):
    return max(t for t in range(16, most + 1, 16) if rows % t == 0)


def fill_spread(e_ref, head_dim, heads):
    channels = e_ref.shape[1]
    row = lax.broadcasted_iota(jnp.int32, (LANES, channels), 0)
    col = lax.broadcasted_iota(jnp.int32, (LANES, channels), 1)
    one = jnp.where((col >= row * head_dim) & (col < (row + 1) * head_dim), 1.0, 0.0).astype(BF16)
    e_ref[0:LANES, :] = one
    e_ref[LANES : 2 * LANES, :] = one


def halves(value):
    high = value.astype(BF16)
    return high, (value - high.astype(F32)).astype(BF16)


def spread(value, e_ref):
    return dot(jnp.concatenate(halves(value), axis=1), e_ref[...])


def head_sums(value, e_ref):
    high, low = halves(value)
    e = e_ref[0:LANES, :]
    return dot(high, e, LAST) + dot(low, e, LAST)


def split_pair(pair):
    lane = lax.broadcasted_iota(jnp.int32, pair.shape, 1)
    zero = jnp.zeros_like(pair)
    half = pair.shape[1] // 2
    return jnp.concatenate([jnp.where(lane < half, pair, zero), jnp.where(lane >= half, pair, zero)], axis=0)


def silu_slope(values, logistic):
    return logistic * (1.0 + values * (1.0 - logistic))


def softplus(v):
    return jnp.maximum(v, 0.0) + jnp.log1p(jnp.exp(-jnp.abs(v)))


def conv_pre(raw_ref, w_ref, b_ref, r0, rows, c0, cols):
    taps = w_ref.shape[0]
    window = raw_ref[pl.ds(r0, rows + HALO), pl.ds(c0, cols)].astype(F32)
    total = jnp.broadcast_to(b_ref[:, pl.ds(c0, cols)], (rows, cols))
    shifts = []
    for k in range(taps):
        start = HALO - taps + 1 + k
        shifts.append(window[start : start + rows])
        total = total + w_ref[k : k + 1, pl.ds(c0, cols)] * shifts[-1]
    return total, shifts


def project_kernel(tok, w_in, gain, conv_w, conv_b, dt_bias, a_log,
                   normed, gate, raw, dt_raw, act, dt, cum, cum_t, loc, dec, e, state):
    ext, d = tok.shape
    inner = gate.shape[1]
    conv_ch = raw.shape[1]
    proj = w_in.shape[1]
    heads = proj - inner - conv_ch
    state_n = (conv_ch - inner) // 2
    length = ext - HALO
    chunks = length // CHUNK
    fill_spread(e, inner // heads, heads)
    dt_raw[...] = jnp.zeros_like(dt_raw)
    rt = tile_of(ext, 192)
    ct = 512

    def norm_rows(i, _):
        rows = pl.ds(pl.multiple_of(i * 16, 16), 16)
        t = tok[rows, :].astype(F32)
        r = lax.rsqrt(jnp.mean(t * t, axis=-1, keepdims=True) + EPSILON)
        normed[rows, :] = (t * r * gain[...]).astype(BF16)
        return 0

    lax.fori_loop(0, ext // 16, norm_rows, 0)

    def proj_rows(i, _):
        rows = pl.ds(pl.multiple_of(i * rt, 16), rt)
        n = normed[rows, :]

        def gate_cols(j, _):
            cols = pl.ds(pl.multiple_of(j * ct, ct), ct)
            gate[rows, cols] = dot(n, w_in[:, cols]).astype(BF16)
            return 0

        def x_cols(j, _):
            cols = pl.ds(pl.multiple_of(j * ct, ct), ct)
            src = pl.ds(pl.multiple_of(inner + j * ct, ct), ct)
            raw[rows, cols] = dot(n, w_in[:, src]).astype(BF16)
            return 0

        lax.fori_loop(0, inner // ct, gate_cols, 0)
        lax.fori_loop(0, inner // ct, x_cols, 0)
        last = dot(n, w_in[:, 2 * inner :])
        raw[rows, inner:] = last[:, : conv_ch - inner].astype(BF16)
        dt_raw[rows, 0:heads] = last[:, conv_ch - inner :].astype(BF16).astype(F32)
        return 0

    lax.fori_loop(0, ext // rt, proj_rows, 0)

    def conv_tile(i, _):
        r0 = pl.multiple_of(i * 64, 64)

        def conv_cols(j, _):
            c0 = pl.multiple_of(j * 256, 256)
            pre, _s = conv_pre(raw, conv_w, conv_b, r0, 64, c0, 256)
            act[pl.ds(r0, 64), pl.ds(c0, 256)] = (pre * jax.nn.sigmoid(pre)).astype(BF16)
            return 0

        return lax.fori_loop(0, conv_ch // 256, conv_cols, 0)

    lax.fori_loop(0, length // 64, conv_tile, 0)

    t_i = lax.broadcasted_iota(jnp.int32, (CHUNK, CHUNK), 0)
    s_i = lax.broadcasted_iota(jnp.int32, (CHUNK, CHUNK), 1)
    tril = jnp.where(t_i >= s_i, 1.0, 0.0)
    rate = -jnp.exp(a_log[...])
    state[...] = jnp.zeros_like(state)
    dec[...] = jnp.zeros_like(dec)

    def chunk(c, _):
        rows = pl.ds(pl.multiple_of(c * CHUNK, CHUNK), CHUNK)
        step = softplus(dt_raw[pl.ds(pl.multiple_of(c * CHUNK + HALO, 16), CHUNK), :] + dt_bias[...])
        dt[rows, :] = step
        running = dot(tril, step * rate, precision=HIGHEST)
        cum[rows, :] = running
        cum_t[c] = running.T
        last = running[CHUNK - 1 : CHUNK, :]
        loc[c] = state[...]
        weight = jnp.exp(last - running) * step
        xw = (act[rows, 0:inner].astype(F32) * spread(weight, e)).astype(BF16)
        b = act[rows, inner : inner + state_n]
        kept = spread(jnp.exp(jnp.broadcast_to(last, (8, LANES))), e)[0:1]
        state[...] = state[...] * kept + dot(b, xw, ROWS)
        dec[...] = dec[...] + last
        return 0

    lax.fori_loop(0, chunks, chunk, 0)
    loc[chunks] = state[...]


def mix_kernel(tok, og, w_out, gate, act, dt, cum, cum_t, loc, enter, gain, skip,
               out, dy, dgate, gw_out, gain_grad, skip_grad, y_dot, states, direct, leave, e, y, xd, gn, dg, acc):
    length, inner = gate.shape[0] - HALO, gate.shape[1]
    state_n = loc.shape[1]
    chunks = length // CHUNK
    pairs = inner // LANES
    fill_spread(e, skip.shape[1] // 1, 0) if False else None
    head_dim = LANES // 2
    fill_spread(e, head_dim, 0)
    t_i = lax.broadcasted_iota(jnp.int32, (CHUNK, CHUNK), 0)
    s_i = lax.broadcasted_iota(jnp.int32, (CHUNK, CHUNK), 1)
    causal = t_i >= s_i
    acc[...] = jnp.zeros_like(acc)
    skip_grad[...] = jnp.zeros_like(skip_grad)
    states[0] = enter[...]

    def chunk(c, carried):
        rows = pl.ds(pl.multiple_of(c * CHUNK, CHUNK), CHUNK)
        running = cum[rows, :]
        step = dt[rows, :]
        last = running[CHUNK - 1 : CHUNK, :]
        grown = spread(jnp.exp(running), e)
        bb = act[rows, inner : inner + state_n]
        cc = act[rows, inner + state_n :]
        scores = dot(cc, bb, LAST)
        s_in = states[c].astype(BF16)
        y[...] = dot(cc, s_in) * grown
        xd[...] = (act[rows, 0:inner].astype(F32) * spread(step, e)).astype(BF16)
        for p in range(pairs):
            cols = slice(p * LANES, (p + 1) * LANES)
            mix = []
            for h in (2 * p, 2 * p + 1):
                gap = running[:, h : h + 1] - cum_t[c, h : h + 1, :]
                mix.append((scores * jnp.exp(jnp.where(causal, gap, -1e30))).astype(BF16))
            y[:, cols] = y[:, cols] + dot(jnp.concatenate(mix, axis=1), split_pair(xd[:, cols]))
        dg[...] = dot(og[rows, :], w_out[...], LAST)

        def rows16(i, _):
            sub = pl.ds(pl.multiple_of(i * 16, 16), 16)
            at = pl.ds(pl.multiple_of(c * CHUNK + i * 16, 16), 16)
            gate_f = gate[pl.ds(pl.multiple_of(c * CHUNK + i * 16 + HALO, 16), 16), :].astype(F32)
            x = act[at, 0:inner].astype(F32)
            mixed = (y[sub, :] + skip[...] * x).astype(BF16).astype(F32)
            logistic = jax.nn.sigmoid(gate_f)
            silu = gate_f * logistic
            gated = mixed * silu
            rms = lax.rsqrt(jnp.mean(gated * gated, axis=-1, keepdims=True) + EPSILON)
            unit = gated * rms
            gn[at, :] = (unit * gain[...]).astype(BF16)
            d_norm = dg[sub, :]
            both = d_norm * unit
            acc[...] = acc[...] + both[0:8] + both[8:16]
            scaled = d_norm * gain[...]
            d_gated = rms * (scaled - unit * jnp.mean(unit * scaled, axis=-1, keepdims=True))
            dy[at, :] = (d_gated * silu).astype(BF16)
            dgate[at, :] = (d_gated * mixed * silu_slope(gate_f, logistic)).astype(BF16)
            return 0

        lax.fori_loop(0, CHUNK // 16, rows16, 0)
        tok_f = tok[pl.ds(pl.multiple_of(c * CHUNK + HALO, 16), CHUNK), :].astype(F32)
        out[rows, :] = (tok_f + dot(gn[rows, :], w_out[...])).astype(BF16)
        dy_f = dy[rows, :].astype(F32)
        direct[c] = dot(cc, (dy_f * grown).astype(BF16), ROWS)
        y_dot[rows, :] = head_sums(dy_f * y[...], e)
        x_sum = head_sums(dy_f * act[rows, 0:inner].astype(F32), e)
        skip_grad[...] = skip_grad[...] + jnp.sum(x_sum, axis=0, keepdims=True)
        total = carried + last
        far = spread(jnp.exp(jnp.broadcast_to(total, (8, LANES))), e)[0:1]
        states[c + 1] = loc[c + 1] + enter[...] * far
        return total

    lax.fori_loop(0, chunks, chunk, jnp.zeros((1, LANES), F32))
    gain_grad[...] = jnp.sum(acc[...], axis=0, keepdims=True)

    leave[...] = jnp.zeros_like(leave)

    def back(i, _):
        c = chunks - 1 - i
        last = cum[pl.ds(pl.multiple_of(c * CHUNK + CHUNK - 8, 8), 8), :]
        leave[...] = leave[...] * spread(jnp.exp(last), e)[7:8] + direct[c]
        return 0

    lax.fori_loop(0, chunks, back, 0)

    def w_rows(i, _):
        cols = pl.ds(pl.multiple_of(i * 256, 256), 256)
        gw_out[cols, :] = dot(gn[:, cols], og[...], ROWS)
        return 0

    lax.fori_loop(0, inner // 256, w_rows, 0)


def back_kernel(raw, dt_raw, act, dt, cum, cum_t, dy, states, direct, leaving, y_dot, conv_w, conv_b, dt_bias, a_log, skip,
                d_pre, d_dt, w_grad, b_grad, bias_grad, rate_grad, e, xd, dxd, d_act, d_state, w_acc):
    length, inner = dy.shape
    conv_ch = raw.shape[1]
    state_n = states.shape[1]
    chunks = length // CHUNK
    pairs = inner // LANES
    fill_spread(e, LANES // 2, 0)
    s_i = lax.broadcasted_iota(jnp.int32, (CHUNK, CHUNK), 0)
    t_i = lax.broadcasted_iota(jnp.int32, (CHUNK, CHUNK), 1)
    causal = t_i >= s_i
    triu = jnp.where(causal, 1.0, 0.0)
    rate = -jnp.exp(a_log[...])
    w_acc[...] = jnp.zeros_like(w_acc)
    bias_grad[...] = jnp.zeros_like(bias_grad)
    rate_grad[...] = jnp.zeros_like(rate_grad)
    d_state[...] = leaving[...]
    d_pre[length:, :] = jnp.zeros((HALO, conv_ch), BF16)

    def chunk(i, _):
        c = chunks - 1 - i
        rows = pl.ds(pl.multiple_of(c * CHUNK, CHUNK), CHUNK)
        running = cum[rows, :]
        step = dt[rows, :]
        last = running[CHUNK - 1 : CHUNK, :]
        ds = d_state[...]
        dsb = ds.astype(BF16)
        bb = act[rows, inner : inner + state_n]
        cc = act[rows, inner + state_n :]
        scores = dot(bb, cc, LAST)
        tail = spread(jnp.exp(last - running), e)
        dxd[...] = dot(bb, dsb) * tail
        x_f = act[rows, 0:inner].astype(F32)
        xd_f = x_f * spread(step, e)
        xd[...] = xd_f.astype(BF16)
        d_scores = jnp.zeros((CHUNK, CHUNK), F32)
        for p in range(pairs):
            cols = slice(p * LANES, (p + 1) * LANES)
            dyp = dy[rows, cols]
            d_mix = dot(split_pair(xd[:, cols]), dyp, LAST)
            mix = []
            for k in range(2):
                h = 2 * p + k
                gap = cum_t[c, h : h + 1, :] - running[:, h : h + 1]
                decay = jnp.exp(jnp.where(causal, gap, -1e30))
                mix.append((scores * decay).astype(BF16))
                d_scores = d_scores + decay * d_mix[k * CHUNK : (k + 1) * CHUNK]
            dxd[:, cols] = dxd[:, cols] + dot(jnp.concatenate(mix, axis=1), split_pair(dyp))
        dsc = d_scores.astype(BF16)
        dy_f = dy[rows, :].astype(F32)
        d_act[:, inner : inner + state_n] = dot(dsc, cc) + dot((xd_f * tail).astype(BF16), dsb, LAST)
        grown = spread(jnp.exp(running), e)
        d_act[:, inner + state_n :] = dot(dsc, bb, ROWS) + dot((dy_f * grown).astype(BF16), states[c].astype(BF16), LAST)
        dxd_f = dxd[...]
        d_act[:, 0:inner] = skip[...] * dy_f + spread(step, e) * dxd_f
        d_step = head_sums(x_f * dxd_f, e)
        base = head_sums(jnp.broadcast_to(jnp.sum(ds * states[c + 1], axis=0, keepdims=True), (8, inner)), e)[0:1]
        d_log = dot(triu, y_dot[rows, :] - step * d_step, precision=HIGHEST) + base
        rate_grad[...] = rate_grad[...] + jnp.sum(d_log * step, axis=0, keepdims=True) * rate
        logistic = jax.nn.sigmoid(dt_raw[pl.ds(pl.multiple_of(c * CHUNK + HALO, 16), CHUNK), :] + dt_bias[...])
        d_raw = (d_step + d_log * rate) * logistic
        d_dt[rows, :] = d_raw
        bias_grad[...] = bias_grad[...] + jnp.sum(d_raw, axis=0, keepdims=True)
        kept = spread(jnp.exp(jnp.broadcast_to(last, (8, LANES))), e)[0:1]
        d_state[...] = ds * kept + direct[c]

        def conv_tile(i, _):
            r0 = pl.multiple_of(c * CHUNK + i * 64, 64)

            def conv_cols(j, _):
                c0 = pl.multiple_of(j * 256, 256)
                pre, shifts = conv_pre(raw, conv_w, conv_b, r0, 64, c0, 256)
                dp = d_act[pl.ds(pl.multiple_of(i * 64, 64), 64), pl.ds(c0, 256)] * silu_slope(pre, jax.nn.sigmoid(pre))
                d_pre[pl.ds(r0, 64), pl.ds(c0, 256)] = dp.astype(BF16)
                for k in range(len(shifts)):
                    w_acc[k, :, pl.ds(c0, 256)] += jnp.sum((dp * shifts[k]).reshape(8, 8, 256), axis=0)
                w_acc[len(shifts), :, pl.ds(c0, 256)] += jnp.sum(dp.reshape(8, 8, 256), axis=0)
                return 0

            return lax.fori_loop(0, conv_ch // 256, conv_cols, 0)

        lax.fori_loop(0, CHUNK // 64, conv_tile, 0)
        return 0

    lax.fori_loop(0, chunks, chunk, 0)
    taps = w_grad.shape[0]
    for k in range(taps):
        w_grad[k : k + 1, :] = jnp.sum(w_acc[k], axis=0, keepdims=True)
    b_grad[...] = jnp.sum(w_acc[taps], axis=0, keepdims=True)


def input_kernel(tok, og, normed, w_in, gain, conv_w, dgate, d_pre, d_dt,
                 in_grad, gw_in, gain_grad, d_raw, dn, acc):
    length, inner = dgate.shape
    ext, d = tok.shape
    conv_ch = d_pre.shape[1]
    proj = w_in.shape[1]
    heads = proj - inner - conv_ch
    taps = conv_w.shape[0]

    def conv_tile(i, _):
        r0 = pl.multiple_of(i * 64, 64)

        def conv_cols(j, _):
            c0 = pl.multiple_of(j * 256, 256)
            window = d_pre[pl.ds(r0, 64 + HALO), pl.ds(c0, 256)].astype(F32)
            total = jnp.zeros((64, 256), F32)
            for k in range(taps):
                off = taps - 1 - k
                total = total + conv_w[k : k + 1, pl.ds(c0, 256)] * window[off : off + 64]
            d_raw[pl.ds(r0, 64), pl.ds(c0, 256)] = total.astype(BF16)
            return 0

        return lax.fori_loop(0, conv_ch // 256, conv_cols, 0)

    lax.fori_loop(0, length // 64, conv_tile, 0)
    d_raw[:, conv_ch : conv_ch + LANES] = d_dt[...].astype(BF16)
    acc[...] = jnp.zeros_like(acc)

    def grad_rows(i, _):
        rows = pl.ds(pl.multiple_of(i * CHUNK, CHUNK), CHUNK)
        total = dot(dgate[rows, :], w_in[:, 0:inner], LAST)
        dn[...] = total + dot(d_raw[rows, 0 : conv_ch + heads], w_in[:, inner:], LAST)

        def rows16(j, _):
            sub = pl.ds(pl.multiple_of(j * 16, 16), 16)
            at = pl.ds(pl.multiple_of(i * CHUNK + j * 16, 16), 16)
            t = tok[pl.ds(pl.multiple_of(i * CHUNK + j * 16 + HALO, 16), 16), :].astype(F32)
            r = lax.rsqrt(jnp.mean(t * t, axis=-1, keepdims=True) + EPSILON)
            unit = t * r
            g = dn[sub, :]
            both = g * unit
            acc[...] = acc[...] + both[0:8] + both[8:16]
            scaled = g * gain[...]
            back = r * (scaled - unit * jnp.mean(unit * scaled, axis=-1, keepdims=True))
            in_grad[at, :] = (og[at, :].astype(F32) + back).astype(in_grad.dtype)
            return 0

        return lax.fori_loop(0, CHUNK // 16, rows16, 0)

    lax.fori_loop(0, length // CHUNK, grad_rows, 0)
    gain_grad[...] = jnp.sum(acc[...], axis=0, keepdims=True)

    def w_rows(i, _):
        cols = pl.ds(pl.multiple_of(i * 128, 128), 128)
        n = normed[pl.ds(HALO, length), cols]
        gw_in[cols, 0:inner] = dot(n, dgate[...], ROWS)
        gw_in[cols, inner:] = dot(n, d_raw[:, 0 : conv_ch + heads], ROWS)
        return 0

    lax.fori_loop(0, d // 128, w_rows, 0)


def vmem_call(kernel, outs, scratch, name):
    spec = pl.BlockSpec(memory_space=pltpu.VMEM)

    def run(*args):
        return pl.pallas_call(
            kernel,
            out_shape=[jax.ShapeDtypeStruct(s, t) for s, t in outs],
            in_specs=[spec] * len(args),
            out_specs=[spec] * len(outs),
            scratch_shapes=[pltpu.VMEM(s, t) for s, t in scratch],
            compiler_params=pltpu.CompilerParams(vmem_limit_bytes=VMEM_LIMIT),
            name=name,
        )(*args)

    return run


def shards(block_in, gain_in, w_in, conv_w, conv_b, dt_bias, a_log, d_skip, gain_out, w_out, out_grad):
    both = ("shard", "head")
    ranges, groups = lax.axis_size("shard"), lax.axis_size("head")
    head_index = lax.axis_index("head")
    seqs, segment, d = block_in.shape
    inner = gain_out.shape[0]
    heads = dt_bias.shape[0]
    conv_ch = conv_b.shape[0]
    taps = conv_w.shape[0]
    state_n = (conv_ch - inner) // 2
    parts = groups // seqs
    length = segment * (groups // parts)
    chunks = length // CHUNK
    ext = length + HALO
    members = [(s, h) for s in range(ranges) for h in range(groups)]
    index = {m: i for i, m in enumerate(members)}

    def after(s, h):
        return (s, h + 1) if (h + 1) % parts else (s + 1, h + 1 - parts)

    forth = [(index[m], index[after(*m)]) for m in members if after(*m) in index]
    back = [(b, a) for a, b in forth]

    def to_ranges(array):
        if parts == 1:
            return lax.all_to_all(array, "head", split_axis=0, concat_axis=1, tiled=True)[0]
        everything = lax.all_gather(array, "head", axis=1, tiled=True)
        mine = lax.dynamic_index_in_dim(everything, head_index // parts, 0, False)
        return lax.dynamic_slice_in_dim(mine, (head_index % parts) * length, length, 0)

    def to_blocks(array):
        if parts == 1:
            return lax.all_to_all(array[None], "head", split_axis=1, concat_axis=0, tiled=True)
        everything = lax.all_gather(array, "head", axis=0, tiled=True).reshape(seqs, groups * segment, -1)
        return lax.dynamic_slice_in_dim(everything, head_index * segment, segment, 1)

    def chain(own, decay, route):
        def hop(_, before):
            return lax.ppermute((decay * before.astype(F32) + own).astype(BF16), both, route)

        return lax.fori_loop(0, ranges * parts - 1, hop, jnp.zeros(own.shape, BF16)).astype(F32)

    full_in = lax.all_gather(w_in, both, axis=0, tiled=True)
    full_out = lax.all_gather(w_out, both, axis=0, tiled=True)
    tok = to_ranges(block_in)
    og = to_ranges(out_grad)
    tok = jnp.concatenate([lax.ppermute(tok[-HALO:], both, forth), tok], axis=0)

    pad = LANES - heads
    gain_in_row, gain_out_row, conv_b_row = gain_in[None], gain_out[None], conv_b[None]
    bias_row = jnp.pad(dt_bias, (0, pad))[None]
    rate_row = jnp.pad(a_log, (0, pad), constant_values=-1e30)[None]
    skip_row = jnp.repeat(d_skip, inner // heads)[None]

    normed, gate, raw, dt_raw, act, dt, cum, cum_t, loc, dec = vmem_call(
        project_kernel,
        [
            ((ext, d), BF16), ((ext, inner), BF16), ((ext, conv_ch), BF16), ((ext, LANES), F32), ((length, conv_ch), BF16),
            ((length, LANES), F32), ((length, LANES), F32), ((chunks, LANES, CHUNK), F32),
            ((chunks + 1, state_n, inner), F32), ((1, LANES), F32),
        ],
        [((2 * LANES, inner), BF16), ((state_n, inner), F32)],
        "project",
    )(tok, full_in, gain_in_row, conv_w, conv_b_row, bias_row, rate_row)

    decay = jnp.repeat(jnp.exp(dec[0, :heads]), inner // heads)[None]
    enter = chain(loc[chunks], decay, forth)

    out, dy, dgate, gw_out, g_gain_out, g_skip, y_dot, states, direct, leave = vmem_call(
        mix_kernel,
        [
            ((length, d), BF16), ((length, inner), BF16), ((length, inner), BF16), ((inner, d), F32), ((1, inner), F32),
            ((1, LANES), F32), ((length, LANES), F32), ((chunks + 1, state_n, inner), F32),
            ((chunks, state_n, inner), F32), ((state_n, inner), F32),
        ],
        [
            ((2 * LANES, inner), BF16), ((CHUNK, inner), F32), ((CHUNK, inner), BF16), ((length, inner), BF16),
            ((CHUNK, inner), F32), ((8, inner), F32),
        ],
        "mix",
    )(tok, og, full_out, gate, act, dt, cum, cum_t, loc, enter, gain_out_row, skip_row)

    leaving = chain(leave, decay, back)

    d_pre, d_dt, g_conv_w, g_conv_b, g_bias, g_rate = vmem_call(
        back_kernel,
        [
            ((ext, conv_ch), BF16), ((length, LANES), F32), ((taps, conv_ch), F32), ((1, conv_ch), F32),
            ((1, LANES), F32), ((1, LANES), F32),
        ],
        [
            ((2 * LANES, inner), BF16), ((CHUNK, inner), BF16), ((CHUNK, inner), F32), ((CHUNK, conv_ch), F32),
            ((state_n, inner), F32), ((taps + 1, 8, conv_ch), F32),
        ],
        "back",
    )(raw, dt_raw, act, dt, cum, cum_t, dy, states, direct, leaving, y_dot, conv_w, conv_b_row, bias_row, rate_row, skip_row)

    d_pre = d_pre.at[length:].set(lax.ppermute(d_pre[:HALO], both, back))

    in_grad, gw_in, g_gain_in = vmem_call(
        input_kernel,
        [((length, d), BF16), ((d, w_in.shape[1]), F32), ((1, d), F32)],
        [((length, conv_ch + LANES), BF16), ((CHUNK, d), F32), ((8, d), F32)],
        "input",
    )(tok, og, normed, full_in, gain_in_row, conv_w, dgate, d_pre, d_dt)

    owned_in = lax.psum_scatter(gw_in, both, scatter_dimension=0, tiled=True)
    owned_out = lax.psum_scatter(gw_out, both, scatter_dimension=0, tiled=True)
    small = lax.psum(
        (g_gain_in[0], g_gain_out[0], g_conv_w, g_conv_b[0], g_bias[0, :heads], g_rate[0, :heads], g_skip[0, :heads]), both
    )
    return (
        to_blocks(out),
        to_blocks(in_grad).astype(F32),
        small[0],
        owned_in,
        small[2],
        small[3],
        small[4],
        small[5],
        small[6],
        small[1],
        owned_out,
    )


def solution(mesh):
    rows, tokens = P(("shard", "head"), None), P(None, ("shard", "head"), None)
    return jax.shard_map(
        shards,
        mesh=mesh,
        in_specs=(tokens, P(), rows, P(), P(), P(), P(), P(), P(), rows, tokens),
        out_specs=(tokens, tokens, P(), rows, P(), P(), P(), P(), P(), P(), rows),
        check_vma=False,
    )
```

```python
import functools

import jax
import jax.numpy as jnp
from jax import lax
from jax.experimental import pallas as pl
from jax.experimental.pallas import tpu as pltpu
from jax.sharding import PartitionSpec as P

F32, BF16 = jnp.float32, jnp.bfloat16
EPSILON = 1e-05
HIGHEST = lax.Precision.HIGHEST
CHUNK = 128
HALO = 16
LANES = 128
VMEM_LIMIT = 60 * 1024 * 1024


def dot(a, b, contract=((1,), (0,)), precision=None):
    return lax.dot_general(a, b, (contract, ((), ())), precision=precision, preferred_element_type=F32)


ROWS = ((0,), (0,))
LAST = ((1,), (1,))


def tile_of(rows, most):
    return max(t for t in range(16, most + 1, 16) if rows % t == 0)


def fill_spread(e_ref, head_dim):
    channels = e_ref.shape[1]
    row = lax.broadcasted_iota(jnp.int32, (LANES, channels), 0)
    col = lax.broadcasted_iota(jnp.int32, (LANES, channels), 1)
    one = jnp.where((col >= row * head_dim) & (col < (row + 1) * head_dim), 1.0, 0.0).astype(BF16)
    e_ref[0:LANES, :] = one
    e_ref[LANES : 2 * LANES, :] = one


def halves(value):
    high = value.astype(BF16)
    return high, (value - high.astype(F32)).astype(BF16)


def spread(value, e_ref):
    return dot(jnp.concatenate(halves(value), axis=1), e_ref[...])


def head_sums(value, e_ref):
    high, low = halves(value)
    e = e_ref[0:LANES, :]
    return dot(high, e, LAST) + dot(low, e, LAST)


def split_pair(pair):
    lane = lax.broadcasted_iota(jnp.int32, pair.shape, 1)
    zero = jnp.zeros_like(pair)
    half = pair.shape[1] // 2
    return jnp.concatenate([jnp.where(lane < half, pair, zero), jnp.where(lane >= half, pair, zero)], axis=0)


def silu_slope(values, logistic):
    return logistic * (1.0 + values * (1.0 - logistic))


def softplus(v):
    return jnp.maximum(v, 0.0) + jnp.log1p(jnp.exp(-jnp.abs(v)))


def conv_pre(raw_ref, w_ref, b_ref, r0, rows, c0, cols):
    taps = w_ref.shape[0]
    window = raw_ref[pl.ds(r0, rows + HALO), pl.ds(c0, cols)].astype(F32)
    total = jnp.broadcast_to(b_ref[:, pl.ds(c0, cols)], (rows, cols))
    shifts = []
    for k in range(taps):
        start = HALO - taps + 1 + k
        shifts.append(window[start : start + rows])
        total = total + w_ref[k : k + 1, pl.ds(c0, cols)] * shifts[-1]
    return total, shifts

MESH = pl.DeviceIdType.MESH
HBM = pl.BlockSpec(memory_space=pl.ANY)
VMEM = pl.BlockSpec(memory_space=pltpu.VMEM)


def aligned(value, multiple):
    return pl.multiple_of(value, multiple)


def send(src, dst, send_sem, recv_sem, to):
    copy = pltpu.make_async_remote_copy(
        src_ref=src, dst_ref=dst, send_sem=send_sem, recv_sem=recv_sem, device_id=to, device_id_type=MESH
    )
    copy.start()
    return copy


def arrived(ref, sem):
    pltpu.make_async_copy(ref, ref, sem).wait()


class Place:
    def __init__(self):
        self.s, self.z = lax.axis_index("shard"), lax.axis_index("head")
        s = self.s
        self.core, self.cx, self.cy = s % 2, (s // 2) % 2, s // 4
        self.s_core = s + 1 - 2 * self.core
        self.s_x = s + 2 - 4 * self.cx
        self.s_y = s + 4 - 8 * self.cy
        self.s_diag = self.s_x + 4 - 8 * self.cy

    def at(self, s=None, z=None):
        return {"shard": self.s if s is None else s, "head": self.z if z is None else z}

    def core_of(self, s):
        return s + 1 - 2 * (s % 2)


def greet(targets, count):
    barrier = pltpu.get_barrier_semaphore()
    for device, condition in targets:
        if condition is None:
            pl.semaphore_signal(barrier, inc=1, device_id=device, device_id_type=MESH)
        else:

            @pl.when(condition)
            def _(device=device):
                pl.semaphore_signal(barrier, inc=1, device_id=device, device_id_type=MESH)

    pl.semaphore_wait(barrier, count)


class Gather:
    SEMS = [
        pltpu.SemaphoreType.DMA((2, 4)),
        pltpu.SemaphoreType.DMA((4,)),
        pltpu.SemaphoreType.DMA((3, 4)),
        pltpu.SemaphoreType.DMA((3, 4)),
        pltpu.SemaphoreType.DMA((4, 4)),
        pltpu.SemaphoreType.DMA((4, 4)),
        pltpu.SemaphoreType.DMA,
    ]

    def __init__(self, place, own, full, sems):
        self.p, self.own, self.full = place, own, full
        self.z_send, self.z_recv, self.send, self.recv, self.c_send, self.c_recv, self.local = sems

    def unit(self, s, z):
        rows = self.own.shape[0]
        return self.full.at[pl.ds(aligned((s * 4 + z) * rows, 8), rows), :]

    def outward(self, src, z):
        p = self.p
        to = self.unit(p.s, z)
        send(src, to, self.send.at[0, z], self.recv.at[0, z], p.at(s=p.s_x))
        send(src, to, self.send.at[1, z], self.recv.at[1, z], p.at(s=p.s_y))
        send(src, to, self.c_send.at[0, z], self.c_recv.at[0, z], p.at(s=p.s_core))

    def start(self):
        p = self.p
        self.keep = pltpu.make_async_copy(self.own, self.unit(p.s, p.z), self.local)
        self.keep.start()
        to = self.unit(p.s, p.z)

        @pl.when(p.z < 3)
        def _():
            send(self.own, to, self.z_send.at[0, p.z], self.z_recv.at[p.z], p.at(z=p.z + 1))

        @pl.when(p.z > 0)
        def _():
            send(self.own, to, self.z_send.at[1, p.z], self.z_recv.at[p.z], p.at(z=p.z - 1))

        self.outward(self.own, p.z)

    def both_sides(self, k, act):
        p = self.p
        if k == 0:
            act(p.z, None)
            return

        @pl.when(p.z >= k)
        def _():
            act(p.z - k, 0)

        @pl.when(p.z + k <= 3)
        def _():
            act(p.z + k, 1)

    def column(self, k):
        p = self.p

        def act(z, side):
            unit = self.unit(p.s, z)
            arrived(unit, self.z_recv.at[z])
            if side == 0:

                @pl.when(p.z < 3)
                def _():
                    send(unit, unit, self.z_send.at[0, z], self.z_recv.at[z], p.at(z=p.z + 1))

            else:

                @pl.when(p.z > 0)
                def _():
                    send(unit, unit, self.z_send.at[1, z], self.z_recv.at[z], p.at(z=p.z - 1))

            self.outward(unit, z)

        self.both_sides(k, act)

    def sideways(self, k):
        p = self.p

        def act(z, side):
            for axis, s in ((0, p.s_x), (1, p.s_y)):
                unit = self.unit(s, z)
                arrived(unit, self.recv.at[axis, z])
                onward = p.s_y if axis == 0 else p.s_x
                turn = z < 2 if axis == 0 else z >= 2

                @pl.when(turn)
                def _(unit=unit, onward=onward):
                    send(unit, unit, self.send.at[2, z], self.recv.at[2, z], p.at(s=onward))

                send(unit, unit, self.c_send.at[1 + axis, z], self.c_recv.at[1 + axis, z], p.at(s=p.s_core))

        self.both_sides(k, act)

    def diagonal(self, k):
        p = self.p

        def act(z, side):
            unit = self.unit(p.s_diag, z)
            arrived(unit, self.recv.at[2, z])
            send(unit, unit, self.c_send.at[3, z], self.c_recv.at[3, z], p.at(s=p.s_core))

        self.both_sides(k, act)

    def steps(self):
        todo = []
        for k in range(1, 4):
            todo.append(functools.partial(self.column, k))
            todo.append(functools.partial(self.sideways, k - 1))
            if k > 1:
                todo.append(functools.partial(self.diagonal, k - 2))
        todo.append(functools.partial(self.sideways, 3))
        todo.append(functools.partial(self.diagonal, 2))
        todo.append(functools.partial(self.diagonal, 3))
        todo.append(self.others)
        return todo

    def others(self):
        p = self.p
        for column, s in enumerate((p.s, p.s_x, p.s_y, p.s_diag)):
            for z in range(4):
                arrived(self.unit(p.core_of(s), z), self.c_recv.at[column, z])
        self.keep.wait()

    def drain(self):
        p = self.p
        for z in range(4):
            unit = self.unit(p.s, z)

            @pl.when((p.z < 3) & (z <= p.z))
            def _(unit=unit, z=z):
                arrived(unit, self.z_send.at[0, z])

            @pl.when((p.z > 0) & (z >= p.z))
            def _(unit=unit, z=z):
                arrived(unit, self.z_send.at[1, z])

            for axis in range(3):
                arrived(unit, self.send.at[axis, z])
            for column in range(4):
                arrived(unit, self.c_send.at[column, z])


class Exchange:
    SEMS = [pltpu.SemaphoreType.DMA((4,)), pltpu.SemaphoreType.DMA((4,)), pltpu.SemaphoreType.DMA]

    def __init__(self, place, blocks, rows, offset, sems):
        self.p, self.blocks, self.rows, self.offset = place, blocks, rows, offset
        self.send, self.recv, self.local = sems

    def part(self, z):
        size = self.blocks.shape[1]
        return self.rows.at[pl.ds(aligned(self.offset + z * size, 16), size), :]

    def start(self):
        p = self.p
        self.keep = pltpu.make_async_copy(self.blocks.at[p.z], self.part(p.z), self.local)
        self.keep.start()
        for k in (1, 2, 3):
            z = (p.z + k) % 4
            send(self.blocks.at[z], self.part(p.z), self.send.at[z], self.recv.at[p.z], p.at(z=z))

    def finish(self):
        p = self.p
        for k in (1, 2, 3):
            z = (p.z + k) % 4
            arrived(self.part(z), self.recv.at[z])
        self.keep.wait()

    def drain(self):
        p = self.p
        for k in (1, 2, 3):
            z = (p.z + k) % 4
            arrived(self.part(z), self.send.at[z])


def project_kernel(tok, w_in, gain, conv_w, conv_b, dt_bias, a_log,
                   normed, gate, raw, dt_raw, act, dt, cum, cum_t, loc, dec, e, state, between=()):
    between = list(between)

    def comm(count=1):
        for _ in range(count):
            if between:
                between.pop(0)()

    ext, d = tok.shape
    inner = gate.shape[1]
    conv_ch = raw.shape[1]
    proj = w_in.shape[1]
    heads = proj - inner - conv_ch
    state_n = (conv_ch - inner) // 2
    length = ext - HALO
    chunks = length // CHUNK
    fill_spread(e, inner // heads)
    dt_raw[...] = jnp.zeros_like(dt_raw)
    rt = tile_of(ext, 192)
    ct = 512

    def norm_rows(i, _):
        rows = pl.ds(pl.multiple_of(i * 16, 16), 16)
        t = tok[rows, :].astype(F32)
        r = lax.rsqrt(jnp.mean(t * t, axis=-1, keepdims=True) + EPSILON)
        normed[rows, :] = (t * r * gain[...]).astype(BF16)
        return 0

    lax.fori_loop(0, ext // 16, norm_rows, 0)

    def proj_rows(i, _):
        rows = pl.ds(i * rt, rt)
        n = normed[rows, :]

        def gate_cols(j, _):
            cols = pl.ds(pl.multiple_of(j * ct, ct), ct)
            gate[rows, cols] = dot(n, w_in[:, cols]).astype(BF16)
            return 0

        def x_cols(j, _):
            cols = pl.ds(pl.multiple_of(j * ct, ct), ct)
            src = pl.ds(pl.multiple_of(inner + j * ct, ct), ct)
            raw[rows, cols] = dot(n, w_in[:, src]).astype(BF16)
            return 0

        lax.fori_loop(0, inner // ct, gate_cols, 0)
        lax.fori_loop(0, inner // ct, x_cols, 0)
        last = dot(n, w_in[:, 2 * inner :])
        raw[rows, inner:] = last[:, : conv_ch - inner].astype(BF16)
        dt_raw[rows, 0:heads] = last[:, conv_ch - inner :].astype(BF16).astype(F32)
        return 0

    for i in range(ext // rt):
        proj_rows(i, 0)
        comm(2)

    def conv_tile(i, _):
        r0 = pl.multiple_of(i * 64, 64)

        def conv_cols(j, _):
            c0 = pl.multiple_of(j * 256, 256)
            pre, _s = conv_pre(raw, conv_w, conv_b, r0, 64, c0, 256)
            act[pl.ds(r0, 64), pl.ds(c0, 256)] = (pre * jax.nn.sigmoid(pre)).astype(BF16)
            return 0

        return lax.fori_loop(0, conv_ch // 256, conv_cols, 0)

    for part in range(4):
        lax.fori_loop(part * length // 256, (part + 1) * length // 256, conv_tile, 0)
        comm()

    t_i = lax.broadcasted_iota(jnp.int32, (CHUNK, CHUNK), 0)
    s_i = lax.broadcasted_iota(jnp.int32, (CHUNK, CHUNK), 1)
    tril = jnp.where(t_i >= s_i, 1.0, 0.0)
    rate = -jnp.exp(a_log[...])
    state[...] = jnp.zeros_like(state)
    dec[...] = jnp.zeros_like(dec)

    def chunk(c, _):
        rows = pl.ds(pl.multiple_of(c * CHUNK, CHUNK), CHUNK)
        step = softplus(dt_raw[pl.ds(pl.multiple_of(c * CHUNK + HALO, 16), CHUNK), :] + dt_bias[...])
        dt[rows, :] = step
        running = dot(tril, step * rate, precision=HIGHEST)
        cum[rows, :] = running
        cum_t[c] = running.T
        last = running[CHUNK - 1 : CHUNK, :]
        loc[c] = state[...]
        weight = jnp.exp(last - running) * step
        xw = (act[rows, 0:inner].astype(F32) * spread(weight, e)).astype(BF16)
        b = act[rows, inner : inner + state_n]
        kept = spread(jnp.exp(jnp.broadcast_to(last, (8, LANES))), e)[0:1]
        state[...] = state[...] * kept + dot(b, xw, ROWS)
        dec[...] = dec[...] + last
        return 0

    lax.fori_loop(0, chunks, chunk, 0)
    loc[chunks] = state[...]
    comm(len(between))


def gather_kernel(blocks, grads, w_in_own, w_out_own, gain, conv_w, conv_b, dt_bias, a_log,
                  tok, og, w_in, w_out, normed, gate, raw, dt_raw, act, dt, cum, cum_t, loc, dec, e, state, *sems):
    p = Place()
    size = blocks.shape[1]
    last = 7
    targets = [(p.at(z=(p.z + k) % 4), None) for k in (1, 2, 3)]
    targets += [(p.at(s=s), None) for s in (p.s_core, p.s_x, p.s_y)]
    halo_out = (p.z == 3) & (p.s < last)
    targets += [(p.at(s=p.s + 1, z=q), halo_out) for q in range(4)]
    targets += [(p.at(s=p.s - 1, z=3), p.s > 0)]
    greet(targets, 6 + jnp.where(p.s > 0, 1, 0) + jnp.where(halo_out, 4, 0))

    n_g, n_x = len(Gather.SEMS), len(Exchange.SEMS)
    first = Gather(p, w_in_own, w_in, sems[:n_g])
    second = Gather(p, w_out_own, w_out, sems[n_g : 2 * n_g])
    tokens = Exchange(p, blocks, tok, HALO, sems[2 * n_g : 2 * n_g + n_x])
    cotangents = Exchange(p, grads, og, 0, sems[2 * n_g + n_x : 2 * n_g + 2 * n_x])
    halo_send, halo_recv = sems[2 * n_g + 2 * n_x :]
    halo = tok.at[0:HALO, :]
    first.start()

    @pl.when(halo_out)
    def _():
        for q in range(4):
            send(blocks.at[q, size - HALO : size, :], halo, halo_send.at[q], halo_recv, p.at(s=p.s + 1, z=q))

    tokens.start()
    for step in first.steps():
        step()
    tokens.finish()

    @pl.when(p.s > 0)
    def _():
        arrived(halo, halo_recv)

    @pl.when(p.s == 0)
    def _():
        tok[0:HALO, :] = jnp.zeros((HALO, tok.shape[1]), tok.dtype)

    second.start()
    cotangents.start()
    project_kernel(tok, w_in, gain, conv_w, conv_b, dt_bias, a_log, normed, gate, raw, dt_raw, act, dt, cum, cum_t, loc, dec,
                   e, state, between=second.steps())
    cotangents.finish()
    first.drain()
    second.drain()
    tokens.drain()
    cotangents.drain()

    @pl.when(halo_out)
    def _():
        for q in range(4):
            arrived(halo, halo_send.at[q])


def mix_kernel(tok, og, w_out, gate, act, dt, cum, cum_t, loc, enter, gain, skip,
               out, dy, dgate, gw_out, gain_grad, skip_grad, y_dot, states, direct, leave, e, y, xd, gn, dg, acc):
    length, inner = gate.shape[0] - HALO, gate.shape[1]
    state_n = loc.shape[1]
    chunks = length // CHUNK
    pairs = inner // LANES
    fill_spread(e, LANES // 2)
    t_i = lax.broadcasted_iota(jnp.int32, (CHUNK, CHUNK), 0)
    s_i = lax.broadcasted_iota(jnp.int32, (CHUNK, CHUNK), 1)
    causal = t_i >= s_i
    acc[...] = jnp.zeros_like(acc)
    skip_grad[...] = jnp.zeros_like(skip_grad)
    states[0] = enter[...]

    def chunk(c, carried):
        rows = pl.ds(pl.multiple_of(c * CHUNK, CHUNK), CHUNK)
        running = cum[rows, :]
        step = dt[rows, :]
        last = running[CHUNK - 1 : CHUNK, :]
        grown = spread(jnp.exp(running), e)
        bb = act[rows, inner : inner + state_n]
        cc = act[rows, inner + state_n :]
        scores = dot(cc, bb, LAST)
        s_in = states[c].astype(BF16)
        y[...] = dot(cc, s_in) * grown
        xd[...] = (act[rows, 0:inner].astype(F32) * spread(step, e)).astype(BF16)
        for p in range(pairs):
            cols = slice(p * LANES, (p + 1) * LANES)
            mix = []
            for h in (2 * p, 2 * p + 1):
                gap = running[:, h : h + 1] - cum_t[c, h : h + 1, :]
                mix.append((scores * jnp.exp(jnp.where(causal, gap, -1e30))).astype(BF16))
            y[:, cols] = y[:, cols] + dot(jnp.concatenate(mix, axis=1), split_pair(xd[:, cols]))
        dg[...] = dot(og[rows, :], w_out[...], LAST)

        def rows16(i, _):
            sub = pl.ds(pl.multiple_of(i * 16, 16), 16)
            at = pl.ds(pl.multiple_of(c * CHUNK + i * 16, 16), 16)
            gate_f = gate[pl.ds(pl.multiple_of(c * CHUNK + i * 16 + HALO, 16), 16), :].astype(F32)
            x = act[at, 0:inner].astype(F32)
            mixed = (y[sub, :] + skip[...] * x).astype(BF16).astype(F32)
            logistic = jax.nn.sigmoid(gate_f)
            silu = gate_f * logistic
            gated = mixed * silu
            rms = lax.rsqrt(jnp.mean(gated * gated, axis=-1, keepdims=True) + EPSILON)
            unit = gated * rms
            gn[at, :] = (unit * gain[...]).astype(BF16)
            d_norm = dg[sub, :]
            both = d_norm * unit
            acc[...] = acc[...] + both[0:8] + both[8:16]
            scaled = d_norm * gain[...]
            d_gated = rms * (scaled - unit * jnp.mean(unit * scaled, axis=-1, keepdims=True))
            dy[at, :] = (d_gated * silu).astype(BF16)
            dgate[at, :] = (d_gated * mixed * silu_slope(gate_f, logistic)).astype(BF16)
            return 0

        lax.fori_loop(0, CHUNK // 16, rows16, 0)
        tok_f = tok[pl.ds(pl.multiple_of(c * CHUNK + HALO, 16), CHUNK), :].astype(F32)
        out[rows, :] = (tok_f + dot(gn[rows, :], w_out[...])).astype(BF16)
        dy_f = dy[rows, :].astype(F32)
        direct[c] = dot(cc, (dy_f * grown).astype(BF16), ROWS)
        y_dot[rows, :] = head_sums(dy_f * y[...], e)
        x_sum = head_sums(dy_f * act[rows, 0:inner].astype(F32), e)
        skip_grad[...] = skip_grad[...] + jnp.sum(x_sum, axis=0, keepdims=True)
        total = carried + last
        far = spread(jnp.exp(jnp.broadcast_to(total, (8, LANES))), e)[0:1]
        states[c + 1] = loc[c + 1] + enter[...] * far
        return total

    lax.fori_loop(0, chunks, chunk, jnp.zeros((1, LANES), F32))
    gain_grad[...] = jnp.sum(acc[...], axis=0, keepdims=True)

    leave[...] = jnp.zeros_like(leave)

    def back(i, _):
        c = chunks - 1 - i
        last = cum[pl.ds(pl.multiple_of(c * CHUNK + CHUNK - 8, 8), 8), :]
        leave[...] = leave[...] * spread(jnp.exp(last), e)[7:8] + direct[c]
        return 0

    lax.fori_loop(0, chunks, back, 0)

    def w_rows(i, _):
        cols = pl.ds(pl.multiple_of(i * 256, 256), 256)
        gw_out[cols, :] = dot(gn[:, cols], og[...], ROWS)
        return 0

    lax.fori_loop(0, inner // 256, w_rows, 0)


def back_kernel(raw, dt_raw, act, dt, cum, cum_t, dy, states, direct, leaving, y_dot, conv_w, conv_b, dt_bias, a_log, skip,
                d_pre, d_dt, w_grad, b_grad, bias_grad, rate_grad, e, xd, dxd, d_act, d_state, w_acc):
    length, inner = dy.shape
    conv_ch = raw.shape[1]
    state_n = states.shape[1]
    chunks = length // CHUNK
    pairs = inner // LANES
    fill_spread(e, LANES // 2)
    s_i = lax.broadcasted_iota(jnp.int32, (CHUNK, CHUNK), 0)
    t_i = lax.broadcasted_iota(jnp.int32, (CHUNK, CHUNK), 1)
    causal = t_i >= s_i
    triu = jnp.where(causal, 1.0, 0.0)
    rate = -jnp.exp(a_log[...])
    w_acc[...] = jnp.zeros_like(w_acc)
    bias_grad[...] = jnp.zeros_like(bias_grad)
    rate_grad[...] = jnp.zeros_like(rate_grad)
    d_state[...] = leaving[...]
    d_pre[length:, :] = jnp.zeros((HALO, conv_ch), BF16)

    def chunk(i, _):
        c = chunks - 1 - i
        rows = pl.ds(pl.multiple_of(c * CHUNK, CHUNK), CHUNK)
        running = cum[rows, :]
        step = dt[rows, :]
        last = running[CHUNK - 1 : CHUNK, :]
        ds = d_state[...]
        dsb = ds.astype(BF16)
        bb = act[rows, inner : inner + state_n]
        cc = act[rows, inner + state_n :]
        scores = dot(bb, cc, LAST)
        tail = spread(jnp.exp(last - running), e)
        dxd[...] = dot(bb, dsb) * tail
        x_f = act[rows, 0:inner].astype(F32)
        xd_f = x_f * spread(step, e)
        xd[...] = xd_f.astype(BF16)
        d_scores = jnp.zeros((CHUNK, CHUNK), F32)
        for p in range(pairs):
            cols = slice(p * LANES, (p + 1) * LANES)
            dyp = dy[rows, cols]
            d_mix = dot(split_pair(xd[:, cols]), dyp, LAST)
            mix = []
            for k in range(2):
                h = 2 * p + k
                gap = cum_t[c, h : h + 1, :] - running[:, h : h + 1]
                decay = jnp.exp(jnp.where(causal, gap, -1e30))
                mix.append((scores * decay).astype(BF16))
                d_scores = d_scores + decay * d_mix[k * CHUNK : (k + 1) * CHUNK]
            dxd[:, cols] = dxd[:, cols] + dot(jnp.concatenate(mix, axis=1), split_pair(dyp))
        dsc = d_scores.astype(BF16)
        dy_f = dy[rows, :].astype(F32)
        d_act[:, inner : inner + state_n] = dot(dsc, cc) + dot((xd_f * tail).astype(BF16), dsb, LAST)
        grown = spread(jnp.exp(running), e)
        d_act[:, inner + state_n :] = dot(dsc, bb, ROWS) + dot((dy_f * grown).astype(BF16), states[c].astype(BF16), LAST)
        dxd_f = dxd[...]
        d_act[:, 0:inner] = skip[...] * dy_f + spread(step, e) * dxd_f
        d_step = head_sums(x_f * dxd_f, e)
        base = head_sums(jnp.broadcast_to(jnp.sum(ds * states[c + 1], axis=0, keepdims=True), (8, inner)), e)[0:1]
        d_log = dot(triu, y_dot[rows, :] - step * d_step, precision=HIGHEST) + base
        rate_grad[...] = rate_grad[...] + jnp.sum(d_log * step, axis=0, keepdims=True) * rate
        logistic = jax.nn.sigmoid(dt_raw[pl.ds(pl.multiple_of(c * CHUNK + HALO, 16), CHUNK), :] + dt_bias[...])
        d_raw = (d_step + d_log * rate) * logistic
        d_dt[rows, :] = d_raw
        bias_grad[...] = bias_grad[...] + jnp.sum(d_raw, axis=0, keepdims=True)
        kept = spread(jnp.exp(jnp.broadcast_to(last, (8, LANES))), e)[0:1]
        d_state[...] = ds * kept + direct[c]

        def conv_tile(i, _):
            r0 = pl.multiple_of(c * CHUNK + i * 64, 64)

            def conv_cols(j, _):
                c0 = pl.multiple_of(j * 256, 256)
                pre, shifts = conv_pre(raw, conv_w, conv_b, r0, 64, c0, 256)
                dp = d_act[pl.ds(pl.multiple_of(i * 64, 64), 64), pl.ds(c0, 256)] * silu_slope(pre, jax.nn.sigmoid(pre))
                d_pre[pl.ds(r0, 64), pl.ds(c0, 256)] = dp.astype(BF16)
                for k in range(len(shifts)):
                    w_acc[k, :, pl.ds(c0, 256)] += jnp.sum((dp * shifts[k]).reshape(8, 8, 256), axis=0)
                w_acc[len(shifts), :, pl.ds(c0, 256)] += jnp.sum(dp.reshape(8, 8, 256), axis=0)
                return 0

            return lax.fori_loop(0, conv_ch // 256, conv_cols, 0)

        lax.fori_loop(0, CHUNK // 64, conv_tile, 0)
        return 0

    lax.fori_loop(0, chunks, chunk, 0)
    taps = w_grad.shape[0]
    for k in range(taps):
        w_grad[k : k + 1, :] = jnp.sum(w_acc[k], axis=0, keepdims=True)
    b_grad[...] = jnp.sum(w_acc[taps], axis=0, keepdims=True)


def input_kernel(tok, og, normed, w_in, gain, conv_w, dgate, d_pre, d_dt,
                 in_grad, gw_in, gain_grad, d_raw, dn, acc):
    length, inner = dgate.shape
    ext, d = tok.shape
    conv_ch = d_pre.shape[1]
    proj = w_in.shape[1]
    heads = proj - inner - conv_ch
    taps = conv_w.shape[0]

    def conv_tile(i, _):
        r0 = pl.multiple_of(i * 64, 64)

        def conv_cols(j, _):
            c0 = pl.multiple_of(j * 256, 256)
            window = d_pre[pl.ds(r0, 64 + HALO), pl.ds(c0, 256)].astype(F32)
            total = jnp.zeros((64, 256), F32)
            for k in range(taps):
                off = taps - 1 - k
                total = total + conv_w[k : k + 1, pl.ds(c0, 256)] * window[off : off + 64]
            d_raw[pl.ds(r0, 64), pl.ds(c0, 256)] = total.astype(BF16)
            return 0

        return lax.fori_loop(0, conv_ch // 256, conv_cols, 0)

    lax.fori_loop(0, length // 64, conv_tile, 0)
    d_raw[:, conv_ch : conv_ch + LANES] = d_dt[...].astype(BF16)
    acc[...] = jnp.zeros_like(acc)

    def grad_rows(i, _):
        rows = pl.ds(pl.multiple_of(i * CHUNK, CHUNK), CHUNK)
        total = dot(dgate[rows, :], w_in[:, 0:inner], LAST)
        dn[...] = total + dot(d_raw[rows, 0 : conv_ch + heads], w_in[:, inner:], LAST)

        def rows16(j, _):
            sub = pl.ds(pl.multiple_of(j * 16, 16), 16)
            at = pl.ds(pl.multiple_of(i * CHUNK + j * 16, 16), 16)
            t = tok[pl.ds(pl.multiple_of(i * CHUNK + j * 16 + HALO, 16), 16), :].astype(F32)
            r = lax.rsqrt(jnp.mean(t * t, axis=-1, keepdims=True) + EPSILON)
            unit = t * r
            g = dn[sub, :]
            both = g * unit
            acc[...] = acc[...] + both[0:8] + both[8:16]
            scaled = g * gain[...]
            back = r * (scaled - unit * jnp.mean(unit * scaled, axis=-1, keepdims=True))
            in_grad[at, :] = (og[at, :].astype(F32) + back).astype(in_grad.dtype)
            return 0

        return lax.fori_loop(0, CHUNK // 16, rows16, 0)

    lax.fori_loop(0, length // CHUNK, grad_rows, 0)
    gain_grad[...] = jnp.sum(acc[...], axis=0, keepdims=True)

    def w_rows(i, _):
        cols = pl.ds(pl.multiple_of(i * 128, 128), 128)
        n = normed[pl.ds(HALO, length), cols]
        gw_in[cols, 0:inner] = dot(n, dgate[...], ROWS)
        gw_in[cols, inner:] = dot(n, d_raw[:, 0 : conv_ch + heads], ROWS)
        return 0

    lax.fori_loop(0, d // 128, w_rows, 0)


def vmem_call(kernel, outs, scratch, name, in_hbm=(), sems=(), collective=None):
    def run(*args):
        params = {} if collective is None else {"collective_id": collective, "has_side_effects": True}
        return pl.pallas_call(
            kernel,
            out_shape=[jax.ShapeDtypeStruct(s, t) for s, t in outs],
            in_specs=[HBM if i in in_hbm else VMEM for i in range(len(args))],
            out_specs=[VMEM] * len(outs),
            scratch_shapes=[pltpu.VMEM(s, t) for s, t in scratch] + list(sems),
            compiler_params=pltpu.CompilerParams(vmem_limit_bytes=VMEM_LIMIT, **params),
            name=name,
        )(*args)

    return run


def shards(block_in, gain_in, w_in, conv_w, conv_b, dt_bias, a_log, d_skip, gain_out, w_out, out_grad):
    both = ("shard", "head")
    ranges, groups = lax.axis_size("shard"), lax.axis_size("head")
    head_index = lax.axis_index("head")
    seqs, segment, d = block_in.shape
    inner = gain_out.shape[0]
    heads = dt_bias.shape[0]
    conv_ch = conv_b.shape[0]
    taps = conv_w.shape[0]
    state_n = (conv_ch - inner) // 2
    parts = groups // seqs
    length = segment * (groups // parts)
    chunks = length // CHUNK
    ext = length + HALO
    members = [(s, h) for s in range(ranges) for h in range(groups)]
    index = {m: i for i, m in enumerate(members)}

    def after(s, h):
        return (s, h + 1) if (h + 1) % parts else (s + 1, h + 1 - parts)

    forth = [(index[m], index[after(*m)]) for m in members if after(*m) in index]
    back = [(b, a) for a, b in forth]

    def to_ranges(array):
        if parts == 1:
            return lax.all_to_all(array, "head", split_axis=0, concat_axis=1, tiled=True)[0]
        everything = lax.all_gather(array, "head", axis=1, tiled=True)
        mine = lax.dynamic_index_in_dim(everything, head_index // parts, 0, False)
        return lax.dynamic_slice_in_dim(mine, (head_index % parts) * length, length, 0)

    def to_blocks(array):
        if parts == 1:
            return lax.all_to_all(array[None], "head", split_axis=1, concat_axis=0, tiled=True)
        everything = lax.all_gather(array, "head", axis=0, tiled=True).reshape(seqs, groups * segment, -1)
        return lax.dynamic_slice_in_dim(everything, head_index * segment, segment, 1)

    def chain(own, decay, route):
        def hop(_, before):
            return lax.ppermute((decay * before.astype(F32) + own).astype(BF16), both, route)

        return lax.fori_loop(0, ranges * parts - 1, hop, jnp.zeros(own.shape, BF16)).astype(F32)

    pad = LANES - heads
    gain_in_row, gain_out_row, conv_b_row = gain_in[None], gain_out[None], conv_b[None]
    bias_row = jnp.pad(dt_bias, (0, pad))[None]
    rate_row = jnp.pad(a_log, (0, pad), constant_values=-1e30)[None]
    skip_row = jnp.repeat(d_skip, inner // heads)[None]

    own_links = (ranges, groups, seqs) == (8, 4, 4)
    project_outs = [
        ((ext, d), BF16), ((ext, inner), BF16), ((ext, conv_ch), BF16), ((ext, LANES), F32), ((length, conv_ch), BF16),
        ((length, LANES), F32), ((length, LANES), F32), ((chunks, LANES, CHUNK), F32),
        ((chunks + 1, state_n, inner), F32), ((1, LANES), F32),
    ]
    project_scratch = [((2 * LANES, inner), BF16), ((state_n, inner), F32)]
    if own_links:
        shapes = [((ext, d), BF16), ((length, d), BF16), ((d, w_in.shape[1]), BF16), ((inner, d), BF16)]
        tok, og, full_in, full_out, *made = vmem_call(
            gather_kernel, shapes + project_outs, project_scratch, "gather", in_hbm=range(4),
            sems=Gather.SEMS * 2 + Exchange.SEMS * 2 + [pltpu.SemaphoreType.DMA((4,)), pltpu.SemaphoreType.DMA], collective=0,
        )(block_in, out_grad, w_in, w_out, gain_in_row, conv_w, conv_b_row, bias_row, rate_row)
    else:
        full_in = lax.all_gather(w_in, both, axis=0, tiled=True)
        full_out = lax.all_gather(w_out, both, axis=0, tiled=True)
        tok = to_ranges(block_in)
        og = to_ranges(out_grad)
        tok = jnp.concatenate([lax.ppermute(tok[-HALO:], both, forth), tok], axis=0)
        made = vmem_call(project_kernel, project_outs, project_scratch, "project")(
            tok, full_in, gain_in_row, conv_w, conv_b_row, bias_row, rate_row
        )
    normed, gate, raw, dt_raw, act, dt, cum, cum_t, loc, dec = made

    decay = jnp.repeat(jnp.exp(dec[0, :heads]), inner // heads)[None]
    enter = chain(loc[chunks], decay, forth)

    out, dy, dgate, gw_out, g_gain_out, g_skip, y_dot, states, direct, leave = vmem_call(
        mix_kernel,
        [
            ((length, d), BF16), ((length, inner), BF16), ((length, inner), BF16), ((inner, d), F32), ((1, inner), F32),
            ((1, LANES), F32), ((length, LANES), F32), ((chunks + 1, state_n, inner), F32),
            ((chunks, state_n, inner), F32), ((state_n, inner), F32),
        ],
        [
            ((2 * LANES, inner), BF16), ((CHUNK, inner), F32), ((CHUNK, inner), BF16), ((length, inner), BF16),
            ((CHUNK, inner), F32), ((8, inner), F32),
        ],
        "mix",
    )(tok, og, full_out, gate, act, dt, cum, cum_t, loc, enter, gain_out_row, skip_row)

    leaving = chain(leave, decay, back)

    d_pre, d_dt, g_conv_w, g_conv_b, g_bias, g_rate = vmem_call(
        back_kernel,
        [
            ((ext, conv_ch), BF16), ((length, LANES), F32), ((taps, conv_ch), F32), ((1, conv_ch), F32),
            ((1, LANES), F32), ((1, LANES), F32),
        ],
        [
            ((2 * LANES, inner), BF16), ((CHUNK, inner), BF16), ((CHUNK, inner), F32), ((CHUNK, conv_ch), F32),
            ((state_n, inner), F32), ((taps + 1, 8, conv_ch), F32),
        ],
        "back",
    )(raw, dt_raw, act, dt, cum, cum_t, dy, states, direct, leaving, y_dot, conv_w, conv_b_row, bias_row, rate_row, skip_row)

    d_pre = d_pre.at[length:].set(lax.ppermute(d_pre[:HALO], both, back))

    in_grad, gw_in, g_gain_in = vmem_call(
        input_kernel,
        [((length, d), BF16), ((d, w_in.shape[1]), F32), ((1, d), F32)],
        [((length, conv_ch + LANES), BF16), ((CHUNK, d), F32), ((8, d), F32)],
        "input",
    )(tok, og, normed, full_in, gain_in_row, conv_w, dgate, d_pre, d_dt)

    owned_in = lax.psum_scatter(gw_in, both, scatter_dimension=0, tiled=True)
    owned_out = lax.psum_scatter(gw_out, both, scatter_dimension=0, tiled=True)
    small = lax.psum(
        (g_gain_in[0], g_gain_out[0], g_conv_w, g_conv_b[0], g_bias[0, :heads], g_rate[0, :heads], g_skip[0, :heads]), both
    )
    return (
        to_blocks(out),
        to_blocks(in_grad).astype(F32),
        small[0],
        owned_in,
        small[2],
        small[3],
        small[4],
        small[5],
        small[6],
        small[1],
        owned_out,
    )


def solution(mesh):
    rows, tokens = P(("shard", "head"), None), P(None, ("shard", "head"), None)
    return jax.shard_map(
        shards,
        mesh=mesh,
        in_specs=(tokens, P(), rows, P(), P(), P(), P(), P(), P(), rows, tokens),
        out_specs=(tokens, tokens, P(), rows, P(), P(), P(), P(), P(), P(), rows),
        check_vma=False,
    )
```

```python
import contextlib
import functools

import jax
import jax.numpy as jnp
from jax import lax
from jax.experimental import pallas as pl
from jax.experimental.pallas import tpu as pltpu
from jax.sharding import PartitionSpec as P

F32, BF16 = jnp.float32, jnp.bfloat16
EPSILON = 1e-05
HIGHEST = lax.Precision.HIGHEST
CHUNK = 128
HALO = 16
LANES = 128
VMEM_LIMIT = 67_043_328


def scope(name):
    return contextlib.nullcontext()


def dot(a, b, contract=((1,), (0,)), precision=None):
    return lax.dot_general(a, b, (contract, ((), ())), precision=precision, preferred_element_type=F32)


ROWS = ((0,), (0,))
LAST = ((1,), (1,))


def tile_of(rows, most):
    return max(t for t in range(16, most + 1, 16) if rows % t == 0)


def fill_spread(e_ref, head_dim):
    channels = e_ref.shape[1]
    row = lax.broadcasted_iota(jnp.int32, (LANES, channels), 0)
    col = lax.broadcasted_iota(jnp.int32, (LANES, channels), 1)
    one = jnp.where((col >= row * head_dim) & (col < (row + 1) * head_dim), 1.0, 0.0).astype(BF16)
    e_ref[0:LANES, :] = one
    e_ref[LANES : 2 * LANES, :] = one


def halves(value):
    high = value.astype(BF16)
    return high, (value - high.astype(F32)).astype(BF16)


def spread(value, e_ref):
    return dot(jnp.concatenate(halves(value), axis=1), e_ref[...])


def head_sums(value, e_ref):
    high, low = halves(value)
    e = e_ref[0:LANES, :]
    return dot(high, e, LAST) + dot(low, e, LAST)


def split_pair(pair):
    lane = lax.broadcasted_iota(jnp.int32, pair.shape, 1)
    zero = jnp.zeros_like(pair)
    half = pair.shape[1] // 2
    return jnp.concatenate([jnp.where(lane < half, pair, zero), jnp.where(lane >= half, pair, zero)], axis=0)


def silu_slope(values, logistic):
    return logistic * (1.0 + values * (1.0 - logistic))


def softplus(v):
    return jnp.maximum(v, 0.0) + jnp.log1p(jnp.exp(-jnp.abs(v)))


def conv_pre(raw_ref, w_ref, b_ref, r0, rows, c0, cols):
    taps = w_ref.shape[0]
    window = raw_ref[pl.ds(r0, rows + HALO), pl.ds(c0, cols)].astype(F32)
    total = jnp.broadcast_to(b_ref[:, pl.ds(c0, cols)], (rows, cols))
    shifts = []
    for k in range(taps):
        start = HALO - taps + 1 + k
        shifts.append(window[start : start + rows])
        total = total + w_ref[k : k + 1, pl.ds(c0, cols)] * shifts[-1]
    return total, shifts

MESH = pl.DeviceIdType.MESH
HBM = pl.BlockSpec(memory_space=pl.ANY)
VMEM = pl.BlockSpec(memory_space=pltpu.VMEM)


def aligned(value, multiple):
    return pl.multiple_of(value, multiple)


def send(src, dst, send_sem, recv_sem, to):
    copy = pltpu.make_async_remote_copy(
        src_ref=src, dst_ref=dst, send_sem=send_sem, recv_sem=recv_sem, device_id=to, device_id_type=MESH
    )
    copy.start()
    return copy


def arrived(ref, sem):
    pltpu.make_async_copy(ref, ref, sem).wait()


class Place:
    def __init__(self):
        self.s, self.z = lax.axis_index("shard"), lax.axis_index("head")
        s = self.s
        self.core, self.cx, self.cy = s % 2, (s // 2) % 2, s // 4
        self.s_core = s + 1 - 2 * self.core
        self.s_x = s + 2 - 4 * self.cx
        self.s_y = s + 4 - 8 * self.cy
        self.s_diag = self.s_x + 4 - 8 * self.cy

    def at(self, s=None, z=None):
        return {"shard": self.s if s is None else s, "head": self.z if z is None else z}

    def core_of(self, s):
        return s + 1 - 2 * (s % 2)


def greet(targets, count):
    barrier = pltpu.get_barrier_semaphore()
    for device, condition in targets:
        if condition is None:
            pl.semaphore_signal(barrier, inc=1, device_id=device, device_id_type=MESH)
        else:

            @pl.when(condition)
            def _(device=device):
                pl.semaphore_signal(barrier, inc=1, device_id=device, device_id_type=MESH)

    pl.semaphore_wait(barrier, count)


class Gather:
    SEMS = [
        pltpu.SemaphoreType.DMA((2, 4)),
        pltpu.SemaphoreType.DMA((4,)),
        pltpu.SemaphoreType.DMA((3, 4)),
        pltpu.SemaphoreType.DMA((3, 4)),
        pltpu.SemaphoreType.DMA((4, 4)),
        pltpu.SemaphoreType.DMA((4, 4)),
        pltpu.SemaphoreType.DMA,
    ]

    def __init__(self, place, own, full, cols, sems, direct=False):
        self.p, self.own, self.full, self.cols, self.direct = place, own.at[:, cols], full, cols, direct
        self.z_send, self.z_recv, self.send, self.recv, self.c_send, self.c_recv, self.local = sems

    def unit(self, s, z):
        rows = self.own.shape[0]
        return self.full.at[pl.ds(aligned((s * 4 + z) * rows, 8), rows), self.cols]

    def outward(self, src, z):
        p = self.p
        to = self.unit(p.s, z)
        send(src, to, self.send.at[0, z], self.recv.at[0, z], p.at(s=p.s_x))
        send(src, to, self.send.at[1, z], self.recv.at[1, z], p.at(s=p.s_y))
        send(src, to, self.c_send.at[0, z], self.c_recv.at[0, z], p.at(s=p.s_core))

    def start(self):
        p = self.p
        to = self.unit(p.s, p.z)
        pltpu.make_async_copy(self.own, to, self.local).start()

        if self.direct:
            for k in (1, 2, 3):
                for z in (p.z - k, p.z + k):

                    @pl.when((z >= 0) & (z <= 3))
                    def _(z=z):
                        send(self.own, to, self.z_send.at[0, z], self.z_recv.at[p.z], p.at(z=z))

        else:

            @pl.when(p.z < 3)
            def _():
                send(self.own, to, self.z_send.at[0, p.z], self.z_recv.at[p.z], p.at(z=p.z + 1))

            @pl.when(p.z > 0)
            def _():
                send(self.own, to, self.z_send.at[1, p.z], self.z_recv.at[p.z], p.at(z=p.z - 1))

        self.outward(self.own, p.z)

    def both_sides(self, k, act):
        p = self.p
        if k == 0:
            act(p.z, None)
            return

        @pl.when(p.z >= k)
        def _():
            act(p.z - k, 0)

        @pl.when(p.z + k <= 3)
        def _():
            act(p.z + k, 1)

    def column(self, k):
        p = self.p

        def act(z, side):
            unit = self.unit(p.s, z)
            arrived(unit, self.z_recv.at[z])
            if self.direct:
                pass
            elif side == 0:

                @pl.when(p.z < 3)
                def _():
                    send(unit, unit, self.z_send.at[0, z], self.z_recv.at[z], p.at(z=p.z + 1))

            else:

                @pl.when(p.z > 0)
                def _():
                    send(unit, unit, self.z_send.at[1, z], self.z_recv.at[z], p.at(z=p.z - 1))

            self.outward(unit, z)

        self.both_sides(k, act)

    def sideways(self, k):
        p = self.p

        def act(z, side):
            for axis, s in ((0, p.s_x), (1, p.s_y)):
                unit = self.unit(s, z)
                arrived(unit, self.recv.at[axis, z])
                onward = p.s_y if axis == 0 else p.s_x
                turn = z < 2 if axis == 0 else z >= 2

                @pl.when(turn)
                def _(unit=unit, onward=onward):
                    send(unit, unit, self.send.at[2, z], self.recv.at[2, z], p.at(s=onward))

                send(unit, unit, self.c_send.at[1 + axis, z], self.c_recv.at[1 + axis, z], p.at(s=p.s_core))

        self.both_sides(k, act)

    def diagonal(self, k):
        p = self.p

        def act(z, side):
            unit = self.unit(p.s_diag, z)
            arrived(unit, self.recv.at[2, z])
            send(unit, unit, self.c_send.at[3, z], self.c_recv.at[3, z], p.at(s=p.s_core))

        self.both_sides(k, act)

    def steps(self):
        todo = []
        for k in range(1, 4):
            todo.append(functools.partial(self.column, k))
            todo.append(functools.partial(self.sideways, k - 1))
            if k > 1:
                todo.append(functools.partial(self.diagonal, k - 2))
        todo.append(functools.partial(self.sideways, 3))
        todo.append(functools.partial(self.diagonal, 2))
        todo.append(functools.partial(self.diagonal, 3))
        todo.append(self.others)
        return todo

    def others(self):
        p = self.p
        for column, s in enumerate((p.s, p.s_x, p.s_y, p.s_diag)):
            for z in range(4):
                arrived(self.unit(p.core_of(s), z), self.c_recv.at[column, z])
        arrived(self.unit(p.s, p.z), self.local)

    def drain(self):
        p = self.p
        for z in range(4):
            unit = self.unit(p.s, z)
            ups = z != p.z if self.direct else (p.z < 3) & (z <= p.z)

            @pl.when(ups)
            def _(unit=unit, z=z):
                arrived(unit, self.z_send.at[0, z])

            if not self.direct:

                @pl.when((p.z > 0) & (z >= p.z))
                def _(unit=unit, z=z):
                    arrived(unit, self.z_send.at[1, z])

            for axis in range(3):
                arrived(unit, self.send.at[axis, z])
            for column in range(4):
                arrived(unit, self.c_send.at[column, z])


class Exchange:
    SEMS = [pltpu.SemaphoreType.DMA((4,)), pltpu.SemaphoreType.DMA((4,)), pltpu.SemaphoreType.DMA]

    def __init__(self, place, src, dst, sems):
        self.p, self.src, self.dst = place, src, dst
        self.send, self.recv, self.local = sems

    def keep(self):
        p = self.p
        pltpu.make_async_copy(self.src(p.z), self.dst(p.z), self.local).start()

    def push(self, z):
        p = self.p
        send(self.src(z), self.dst(p.z), self.send.at[z], self.recv.at[p.z], p.at(z=z))

    def push_next(self, k):
        self.push((self.p.z + k) % 4)

    def give(self, z):
        pl.when(z == self.p.z)(self.keep)

        @pl.when(z != self.p.z)
        def _():
            self.push(z)

    def take(self, k):
        z = (self.p.z + 4 - k) % 4
        arrived(self.dst(z), self.local if k == 0 else self.recv.at[z])
        return z

    def finish(self):
        for k in range(4):
            self.take(k)

    def drain(self):
        p = self.p
        for k in (1, 2, 3):
            z = (p.z + k) % 4
            arrived(self.src(z), self.send.at[z])


class Chain:
    SEMS = [pltpu.SemaphoreType.DMA((3,))] * 2 + [pltpu.SemaphoreType.DMA((3, 2))] * 2

    @staticmethod
    def buffers(state_n, inner):
        half = inner // 2
        own = [((state_n, inner), BF16), ((2, state_n, half), BF16)]
        return own, [((5, state_n, half), BF16), ((5, 8, LANES), F32)]

    def __init__(self, place, own, decay, enter, e, forward, buffers, sems):
        self.p, self.own, self.decay, self.enter, self.e, self.forward = place, own, decay, enter, e, forward
        self.rounded, self.made, self.landed, self.decays = buffers
        self.c_send, self.c_recv, self.send, self.recv = sems
        self.half = self.made.shape[2]
        p = place
        self.first = p.core == 0 if forward else p.core == 1
        self.early_x = p.cx == 0 if forward else p.cx == 1
        self.early_y = p.cy == 0 if forward else p.cy == 1
        self.mine = pl.ds(aligned(p.core * self.half, LANES), self.half)
        self.theirs = pl.ds(aligned((1 - p.core) * self.half, LANES), self.half)

    def clear(self):
        self.landed[0:3] = jnp.zeros((3,) + self.landed.shape[1:], BF16)
        self.decays[0:3] = jnp.zeros((3,) + self.decays.shape[1:], F32)

    def by_rows(self, body):
        def step(i, _):
            body(pl.ds(aligned(i * 16, 16), 16))
            return 0

        lax.fori_loop(0, self.own.shape[0] // 16, step, 0)

    def start(self):
        p = self.p

        def body(rows):
            self.rounded[rows, :] = self.own[rows, :].astype(BF16)

        self.by_rows(body)
        to = p.at(s=p.s_core)
        send(self.decay, self.decays.at[3], self.c_send.at[1], self.c_recv.at[1], to)
        send(self.rounded.at[:, self.theirs], self.landed.at[3], self.c_send.at[0], self.c_recv.at[0], to)

    def factor(self, logs):
        return spread(jnp.exp(logs), self.e.at[:, self.mine])[0:1]

    def ordered(self, rows):
        own, other = self.rounded[rows, self.mine].astype(F32), self.landed[3, rows, :].astype(F32)
        return jnp.where(self.first, own, other), jnp.where(self.first, other, own)

    def targets(self):
        p = self.p
        return ((0, self.early_x, p.s_x), (1, self.early_y, p.s_y), (2, self.early_y, p.s_diag))

    def chip(self):
        p = self.p
        arrived(self.decays.at[3], self.c_recv.at[1])
        arrived(self.landed.at[3], self.c_recv.at[0])
        own, other = self.decay[...], self.decays[3]
        self.decays[4] = own + other
        second = self.factor(jnp.where(self.first, other, own))

        def body(rows):
            a, b = self.ordered(rows)
            self.made[0, rows, :] = (second * a + b).astype(BF16)

        self.by_rows(body)
        for slot, early, s in self.targets():

            @pl.when(early)
            def _(slot=slot, s=s):
                send(self.decays.at[4], self.decays.at[slot], self.send.at[slot, 1], self.recv.at[slot, 1], p.at(s=s))
                send(self.made.at[0], self.landed.at[slot], self.send.at[slot, 0], self.recv.at[slot, 0], p.at(s=s))

    def enter_chip(self):
        p = self.p
        for slot, early, _s in self.targets():

            @pl.when(jnp.logical_not(early))
            def _(slot=slot):
                arrived(self.decays.at[slot], self.recv.at[slot, 1])
                arrived(self.landed.at[slot], self.recv.at[slot, 0])

        fx, fy, fd = (self.factor(self.decays[k]) for k in range(3))
        own, other = self.decay[...], self.decays[3]
        first = self.factor(jnp.where(self.first, own, other))

        def body(rows):
            x, y, d = (self.landed[k, rows, :].astype(F32) for k in range(3))
            chip = x + fx * jnp.where(self.early_x, d + fd * y, y + fy * d)
            second = first * chip + self.ordered(rows)[0]
            self.enter[rows, self.mine] = jnp.where(self.first, chip, second)
            self.made[1, rows, :] = jnp.where(self.first, second, chip).astype(BF16)

        self.by_rows(body)
        send(self.made.at[1], self.landed.at[4], self.c_send.at[2], self.c_recv.at[2], p.at(s=p.s_core))

    def finish(self):
        arrived(self.landed.at[4], self.c_recv.at[2])

        def body(rows):
            self.enter[rows, self.theirs] = self.landed[4, rows, :].astype(F32)

        self.by_rows(body)

    def drain(self):
        arrived(self.landed.at[3], self.c_send.at[0])
        arrived(self.decays.at[3], self.c_send.at[1])
        arrived(self.landed.at[4], self.c_send.at[2])
        for slot, early, _s in self.targets():

            @pl.when(early)
            def _(slot=slot):
                arrived(self.landed.at[slot], self.send.at[slot, 0])
                arrived(self.decays.at[slot], self.send.at[slot, 1])


class Reduce:
    SEMS = [pltpu.SemaphoreType.DMA((4,))] * 2 + [pltpu.SemaphoreType.DMA((2, 2))] * 2 + [pltpu.SemaphoreType.DMA((4,))] * 2

    @staticmethod
    def buffers(unit, cols):
        return [
            ((4, 4 * unit, cols), BF16), ((2, 2 * unit, cols), BF16), ((2, 4 * unit, cols), BF16), ((4, unit, cols), BF16),
        ]

    def __init__(self, place, grad, owned, cols, buffers, sems):
        self.p, self.grad, self.owned, self.cols = place, grad, owned, cols
        self.pair, self.turn, self.side, self.line = buffers
        self.c_send, self.c_recv, self.send, self.recv, self.z_send, self.z_recv = sems
        self.unit = owned.shape[0]
        p = place
        self.columns = (p.s, p.s_x, p.s_y, p.s_diag)

    def bundle(self, s, first=0, units=4):
        return self.grad.at[pl.ds(aligned((s * 4 + first) * self.unit, 8), units * self.unit), :]

    def cross(self, k):
        p = self.p
        send(
            self.bundle(p.core_of(self.columns[k])), self.pair.at[k], self.c_send.at[k], self.c_recv.at[k], p.at(s=p.s_core)
        )

    def add(self, k, others):
        base = self.columns[k] * 4 * self.unit
        size = 16

        def run(lo, hi, refs):
            def step(i, _):
                at = pl.ds(aligned(base + i * size, 16), size)
                total = self.grad[at, :].astype(F32)
                for ref, start in refs:
                    total = total + ref[pl.ds(aligned(i * size - start, 16), size), :].astype(F32)
                self.grad[at, :] = total.astype(BF16)
                return 0

            lax.fori_loop(lo // size, hi // size, step, 0)

        cuts = sorted({0, 4 * self.unit} | {start for _r, start in others} | {start + r.shape[0] for r, start in others})
        for lo, hi in zip(cuts[:-1], cuts[1:]):
            run(lo, hi, [(r, start) for r, start in others if start <= lo and hi <= start + r.shape[0]])

    def diagonal(self):
        p = self.p
        arrived(self.pair.at[3], self.c_recv.at[3])
        self.add(3, [(self.pair.at[3], 0)])
        send(self.bundle(p.s_diag, 0, 2), self.turn.at[0], self.send.at[0, 0], self.recv.at[0, 0], p.at(s=p.s_x))
        send(self.bundle(p.s_diag, 2, 2), self.turn.at[1], self.send.at[0, 1], self.recv.at[0, 1], p.at(s=p.s_y))

    def sideways(self, axis):
        p = self.p
        came = 1 - axis
        arrived(self.pair.at[1 + axis], self.c_recv.at[1 + axis])
        arrived(self.turn.at[came], self.recv.at[0, came])
        self.add(1 + axis, [(self.pair.at[1 + axis], 0), (self.turn.at[came], 2 * self.unit * came)])
        s = self.columns[1 + axis]
        send(self.bundle(s), self.side.at[axis], self.send.at[1, axis], self.recv.at[1, axis], p.at(s=s))

    def column(self):
        p = self.p
        arrived(self.pair.at[0], self.c_recv.at[0])
        for axis in range(2):
            arrived(self.side.at[axis], self.recv.at[1, axis])
        self.add(0, [(self.pair.at[0], 0), (self.side.at[0], 0), (self.side.at[1], 0)])
        for k in (1, 2, 3):
            z = (p.z + k) % 4
            send(self.bundle(p.s, z, 1), self.line.at[p.z], self.z_send.at[z], self.z_recv.at[p.z], p.at(z=z))

    def own(self):
        p = self.p
        others = [(p.z + k) % 4 for k in (1, 2, 3)]
        for z in others:
            arrived(self.line.at[z], self.z_recv.at[z])
        base = (p.s * 4 + p.z) * self.unit
        for i in range(self.unit // 8):
            total = self.grad[pl.ds(aligned(base + i * 8, 8), 8), :].astype(F32)
            for z in others:
                total = total + self.line[z, i * 8 : i * 8 + 8, :].astype(F32)
            self.owned[i * 8 : i * 8 + 8, self.cols] = total

    def drain(self):
        p = self.p
        for k in range(4):
            arrived(self.pair.at[k], self.c_send.at[k])
        for axis in range(2):
            arrived(self.turn.at[axis], self.send.at[0, axis])
            arrived(self.side.at[axis], self.send.at[1, axis])
        for k in (1, 2, 3):
            z = (p.z + k) % 4
            arrived(self.line.at[z], self.z_send.at[z])


class Total:
    SEMS = [pltpu.SemaphoreType.DMA((6,))] * 2

    def __init__(self, place, stages, landed, sems):
        self.p, self.stages, self.landed = place, stages, landed
        self.send, self.recv = sems

    def push(self, k):
        p = self.p
        if k < 3:
            s = (p.s_core, p.s_x, p.s_y)[k]
            send(self.stages.at[k], self.landed.at[k], self.send.at[k], self.recv.at[k], p.at(s=s))
        else:
            for j in (1, 2, 3):
                z = (p.z + j) % 4
                send(self.stages.at[3], self.landed.at[2 + 4 - j], self.send.at[2 + j], self.recv.at[2 + 4 - j], p.at(z=z))

    def take(self, k):
        arrived(self.landed.at[k], self.recv.at[k])
        self.stages[k + 1] = self.stages[k] + self.landed[k]

    def finish(self, out):
        for j in (3, 4, 5):
            arrived(self.landed.at[j], self.recv.at[j])
        out[...] = (self.stages[3] + self.landed[3]) + (self.landed[4] + self.landed[5])

    def drain(self):
        for k in range(6):
            arrived(self.landed.at[k], self.send.at[k])


class Refs:
    def __init__(self, names, refs):
        self.__dict__.update(zip(names, refs))


def at_step(i, hooks):
    for k, hook in enumerate(hooks):
        if hook is not None:
            pl.when(i == k)(hook)


def chunk_rows(c, offset=0, rows=CHUNK):
    return pl.ds(aligned(c * CHUNK + offset, 16), rows)


def loop(count, body, start=0):
    def step(i, _):
        body(i)
        return 0

    lax.fori_loop(start, count, step, 0)


def project_block(r, c, halo=False):
    d = r.tok.shape[1]
    conv_ch = r.raw.shape[1]
    inner = r.e.shape[1]
    heads = r.w_in.shape[1] - inner - conv_ch
    ct = 512

    def norm(at):
        t = r.tok[at, :].astype(F32)
        scale = lax.rsqrt(jnp.mean(t * t, axis=-1, keepdims=True) + EPSILON)
        r.normed[at, :] = (t * scale * r.gain_in[...]).astype(BF16)

    loop(CHUNK // 32, lambda i: norm(pl.ds(aligned(c * CHUNK + HALO + i * 32, 16), 32)))
    rows = chunk_rows(c, HALO)
    n = r.normed[rows, :]
    if halo:
        norm(slice(0, HALO))
        n = jnp.concatenate([r.normed[0:HALO, :], n], axis=0)
    skip = HALO if halo else 0

    def x_cols(j):
        cols = pl.ds(aligned(j * ct, ct), ct)
        made = dot(n, r.w_in[:, pl.ds(aligned(inner + j * ct, ct), ct)]).astype(BF16)
        r.raw[rows, cols] = made[skip:]
        if halo:
            r.raw[0:HALO, cols] = made[:HALO]

    loop(inner // ct, x_cols)
    last = dot(n, r.w_in[:, 2 * inner :])
    made = last[:, : conv_ch - inner].astype(BF16)
    r.raw[rows, inner:] = made[skip:]
    if halo:
        r.raw[0:HALO, inner:] = made[:HALO]
    r.dt_raw[chunk_rows(c), 0:heads] = last[skip:, conv_ch - inner :].astype(BF16).astype(F32)


def conv_act(r, hooks=()):
    length, conv_ch = r.act.shape[0], r.raw.shape[1]

    def conv_tile(i):
        r0 = aligned(i * 64, 64)

        def conv_cols(j):
            c0 = aligned(j * 256, 256)
            pre, _s = conv_pre(r.raw, r.conv_w, r.conv_b, r0, 64, c0, 256)
            r.act[pl.ds(r0, 64), pl.ds(c0, 256)] = (pre * jax.nn.sigmoid(pre)).astype(BF16)

        loop(conv_ch // 256, conv_cols)
        at_step(i, hooks)

    loop(length // 64, conv_tile)


def scan_states(r, hooks=()):
    conv_ch = r.raw.shape[1]
    inner = r.e.shape[1]
    state_n = (conv_ch - inner) // 2
    chunks = r.act.shape[0] // CHUNK
    t_i = lax.broadcasted_iota(jnp.int32, (CHUNK, CHUNK), 0)
    s_i = lax.broadcasted_iota(jnp.int32, (CHUNK, CHUNK), 1)
    tril = jnp.where(t_i >= s_i, 1.0, 0.0)
    rate = -jnp.exp(r.a_log[...])
    r.state[...] = jnp.zeros_like(r.state)
    r.decay[...] = jnp.zeros_like(r.decay)

    def chunk(c):
        rows = chunk_rows(c)
        step = softplus(r.dt_raw[rows, :] + r.dt_bias[...])
        r.dt[rows, :] = step
        running = dot(tril, step * rate, precision=HIGHEST)
        r.cum[rows, :] = running
        r.cum_t[c] = running.T
        last = running[CHUNK - 1 : CHUNK, :]
        r.states[c] = r.state[...]
        weight = jnp.exp(last - running) * step
        xw = (r.act[rows, 0:inner].astype(F32) * spread(weight, r.e)).astype(BF16)
        b = r.act[rows, inner : inner + state_n]
        kept = spread(jnp.exp(jnp.broadcast_to(last, (8, LANES))), r.e)[0:1]
        r.state[...] = r.state[...] * kept + dot(b, xw, ROWS)
        r.decay[...] = r.decay[...] + last
        at_step(c, hooks)

    loop(chunks, chunk)
    r.states[chunks] = r.state[...]


def project_gate(r, hooks=()):
    ct = 512

    def gate_rows(i):
        n = r.normed[chunk_rows(i, HALO), :]

        def gate_cols(j):
            cols = pl.ds(aligned(j * ct, ct), ct)
            r.gate[chunk_rows(i), cols] = dot(n, r.w_in[:, cols]).astype(BF16)

        loop(r.gate.shape[1] // ct, gate_cols)

        def turn(k):
            cols = pl.ds(aligned(k * 128, 128), 128)
            r.normed_t[cols, chunk_rows(i)] = r.normed[chunk_rows(i, HALO), cols].T

        loop(r.normed_t.shape[0] // 128, turn)
        at_step(i, hooks)

    loop(r.gate.shape[0] // CHUNK, gate_rows)


def mix_inside(r):
    length, inner = r.gate.shape
    state_n = r.states.shape[1]
    t_i = lax.broadcasted_iota(jnp.int32, (CHUNK, CHUNK), 0)
    s_i = lax.broadcasted_iota(jnp.int32, (CHUNK, CHUNK), 1)
    causal = t_i >= s_i

    def chunk(c):
        rows = chunk_rows(c)
        running = r.cum[rows, :]
        scores = dot(r.act[rows, inner + state_n : inner + 2 * state_n], r.act[rows, inner : inner + state_n], LAST)
        r.xd[...] = (r.act[rows, 0:inner].astype(F32) * spread(r.dt[rows, :], r.e)).astype(BF16)
        for p in range(inner // LANES):
            cols = slice(p * LANES, (p + 1) * LANES)
            mix = []
            for h in (2 * p, 2 * p + 1):
                gap = running[:, h : h + 1] - r.cum_t[c, h : h + 1, :]
                mix.append((scores * jnp.exp(jnp.where(causal, gap, -1e30))).astype(BF16))
            r.y[c, :, cols] = dot(jnp.concatenate(mix, axis=1), split_pair(r.xd[:, cols]))

    loop(length // CHUNK, chunk)


def out_cotangent(r, c):
    r.dxd[c] = dot(r.og[chunk_rows(c), :], r.w_out[...], LAST)


def mix_outside(r, give=None):
    length, inner = r.gate.shape
    state_n = r.states.shape[1]
    chunks = length // CHUNK
    r.acc[...] = jnp.zeros_like(r.acc)

    def chunk(c, total):
        rows = chunk_rows(c)
        running = r.cum[rows, :]
        last = running[CHUNK - 1 : CHUNK, :]
        with scope("mo_state"):
            grown = spread(jnp.exp(running), r.e)
            cc = r.act[rows, inner + state_n : inner + 2 * state_n]
            far = spread(jnp.exp(jnp.broadcast_to(total, (8, LANES))), r.e)[0:1]
            s_in = r.states[c] + r.enter[...] * far
            r.states[c] = s_in
            r.y[c] = r.y[c] + dot(cc, s_in.astype(BF16)) * grown

        def rows16(i):
            sub = pl.ds(aligned(i * 16, 16), 16)
            at = pl.ds(aligned(c * CHUNK + i * 16, 16), 16)
            gate_f = r.gate[at, :].astype(F32)
            x = r.act[at, 0:inner].astype(F32)
            mixed = (r.y[c, sub, :] + r.skip[...] * x).astype(BF16).astype(F32)
            logistic = jax.nn.sigmoid(gate_f)
            silu = gate_f * logistic
            gated = mixed * silu
            rms = lax.rsqrt(jnp.mean(gated * gated, axis=-1, keepdims=True) + EPSILON)
            unit = gated * rms
            r.gn[sub, :] = (unit * r.gain_out[...]).astype(BF16)
            d_norm = r.dxd[c, sub, :]
            both = d_norm * unit
            r.acc[...] = r.acc[...] + both[0:8] + both[8:16]
            scaled = d_norm * r.gain_out[...]
            d_gated = rms * (scaled - unit * jnp.mean(unit * scaled, axis=-1, keepdims=True))
            r.dy[at, :] = (d_gated * silu).astype(BF16)
            r.gate[at, :] = (d_gated * mixed * silu_slope(gate_f, logistic)).astype(BF16)

        with scope("mo_elem"):
            loop(CHUNK // 16, rows16)
        with scope("mo_out"):
            tok_f = r.tok[chunk_rows(c, HALO), :].astype(F32)
            r.out[rows, :] = (tok_f + dot(r.gn[...], r.w_out[...])).astype(BF16)
            if give is not None:
                give(c)

        def turn(k):
            cols = pl.ds(aligned(k * 128, 128), 128)
            r.gn_t[cols, rows] = r.gn[:, cols].T

        with scope("mo_turn"):
            loop(inner // 128, turn)
        with scope("mo_direct"):
            r.dxd[c] = dot(cc, (r.dy[rows, :].astype(F32) * grown).astype(BF16), ROWS)
        return total + last

    total = lax.fori_loop(0, chunks, chunk, jnp.zeros((1, LANES), F32))
    far = spread(jnp.exp(jnp.broadcast_to(total, (8, LANES))), r.e)[0:1]
    r.states[chunks] = r.states[chunks] + r.enter[...] * far
    r.small[5:6, 0:inner] = jnp.sum(r.acc[...], axis=0, keepdims=True)
    r.leave[...] = jnp.zeros_like(r.leave)

    def back(i):
        c = chunks - 1 - i
        last = r.cum[pl.ds(aligned(c * CHUNK + CHUNK - 8, 8), 8), :]
        r.leave[...] = r.leave[...] * spread(jnp.exp(last), r.e)[7:8] + r.dxd[c]

    with scope("mo_leave"):
        loop(chunks, back)


def out_weights(r):
    def w_rows(i):
        rows = pl.ds(aligned(i * 256, 256), 256)
        r.gw_out[rows, :] = dot(r.gn_t[rows, :], r.og[...]).astype(r.gw_out.dtype)

    loop(r.gw_out.shape[0] // 256, w_rows)


def back_inside(r, hooks=()):
    length, inner = r.dy.shape
    state_n = r.states.shape[1]
    s_i = lax.broadcasted_iota(jnp.int32, (CHUNK, CHUNK), 0)
    t_i = lax.broadcasted_iota(jnp.int32, (CHUNK, CHUNK), 1)
    causal = t_i >= s_i
    r.skip_acc[...] = jnp.zeros_like(r.skip_acc)

    def chunk(c):
        rows = chunk_rows(c)
        with scope("bi_sums"):
            dy_f = r.dy[rows, :].astype(F32)
            x_f = r.act[rows, 0:inner].astype(F32)
            r.y_dot[rows, :] = head_sums(dy_f * r.y[c], r.e)
            r.skip_acc[...] = r.skip_acc[...] + jnp.sum(head_sums(dy_f * x_f, r.e), axis=0, keepdims=True)
            r.y[c] = r.dxd[c]
        running = r.cum[rows, :]
        bb = r.act[rows, inner : inner + state_n]
        scores = dot(bb, r.act[rows, inner + state_n : inner + 2 * state_n], LAST)
        r.xd[...] = (x_f * spread(r.dt[rows, :], r.e)).astype(BF16)
        d_scores = jnp.zeros((CHUNK, CHUNK), F32)
        with scope("bi_pairs"):
            for p in range(inner // LANES):
                cols = slice(p * LANES, (p + 1) * LANES)
                dyp = r.dy[rows, cols]
                d_mix = dot(split_pair(r.xd[:, cols]), dyp, LAST)
                mix = []
                for k in range(2):
                    h = 2 * p + k
                    gap = r.cum_t[c, h : h + 1, :] - running[:, h : h + 1]
                    decay = jnp.exp(jnp.where(causal, gap, -1e30))
                    mix.append((scores * decay).astype(BF16))
                    d_scores = d_scores + decay * d_mix[k * CHUNK : (k + 1) * CHUNK]
                r.dxd[c, :, cols] = dot(jnp.concatenate(mix, axis=1), split_pair(dyp))
        with scope("bi_c"):
            dsc = d_scores.astype(BF16)
            r.d_scores[c] = dsc
            r.xd[...] = (dy_f * spread(jnp.exp(running), r.e)).astype(BF16)
            r.d_c[rows, :] = dot(dsc, bb, ROWS) + dot(r.xd[...], r.states[c].astype(BF16), LAST)
        at_step(c, hooks)

    loop(length // CHUNK, chunk)
    d = r.tok.shape[1]
    r.small[6:7, d + 2 * LANES : d + 3 * LANES] = r.skip_acc[...]


def back_outside(r, after=None):
    length, inner = r.dy.shape
    conv_ch = r.raw.shape[1]
    state_n = r.states.shape[1]
    chunks = length // CHUNK
    s_i = lax.broadcasted_iota(jnp.int32, (CHUNK, CHUNK), 0)
    t_i = lax.broadcasted_iota(jnp.int32, (CHUNK, CHUNK), 1)
    triu = jnp.where(t_i >= s_i, 1.0, 0.0)
    rate = -jnp.exp(r.a_log[...])
    r.w_acc[...] = jnp.zeros_like(r.w_acc)
    r.bias_acc[...] = jnp.zeros_like(r.bias_acc)
    r.rate_acc[...] = jnp.zeros_like(r.rate_acc)
    taps = r.conv_w.shape[0]

    def chunk(i):
        c = chunks - 1 - i
        rows = chunk_rows(c)
        running = r.cum[rows, :]
        step = r.dt[rows, :]
        last = running[CHUNK - 1 : CHUNK, :]
        with scope("bo_dots"):
            ds = r.leaving[...]
            dsb = ds.astype(BF16)
            bb = r.act[rows, inner : inner + state_n]
            cc = r.act[rows, inner + state_n : inner + 2 * state_n]
            tail = spread(jnp.exp(last - running), r.e)
            step_ch = spread(step, r.e)
            x_f = r.act[rows, 0:inner].astype(F32)
            r.wide[:, inner : inner + state_n] = dot(r.d_scores[c], cc) + dot((x_f * step_ch * tail).astype(BF16), dsb, LAST)
            r.wide[:, inner + state_n : inner + 2 * state_n] = r.d_c[rows, :]
        with scope("bo_sums"):
            dxd = r.dxd[c] + dot(bb, dsb) * tail
            r.wide[:, 0:inner] = r.skip[...] * r.dy[rows, :].astype(F32) + step_ch * dxd
            d_step = head_sums(x_f * dxd, r.e)
            base = head_sums(jnp.broadcast_to(jnp.sum(ds * r.states[c + 1], axis=0, keepdims=True), (8, inner)), r.e)[0:1]
            d_log = dot(triu, r.y_dot[rows, :] - step * d_step, precision=HIGHEST) + base
            r.rate_acc[...] = r.rate_acc[...] + jnp.sum(d_log * step, axis=0, keepdims=True) * rate
            logistic = jax.nn.sigmoid(r.dt_raw[rows, :] + r.dt_bias[...])
            d_raw = (d_step + d_log * rate) * logistic
            r.d_dt[rows, :] = d_raw.astype(BF16)
            r.bias_acc[...] = r.bias_acc[...] + jnp.sum(d_raw, axis=0, keepdims=True)
            kept = spread(jnp.exp(jnp.broadcast_to(last, (8, LANES))), r.e)[0:1]
            r.leaving[...] = ds * kept + r.y[c]

        def conv_tile(k):
            r0 = aligned(c * CHUNK + k * 64, 64)

            def conv_cols(j):
                c0 = aligned(j * 256, 256)
                pre, shifts = conv_pre(r.raw, r.conv_w, r.conv_b, r0, 64, c0, 256)
                dp = r.wide[pl.ds(aligned(k * 64, 64), 64), pl.ds(c0, 256)] * silu_slope(pre, jax.nn.sigmoid(pre))
                r.d_pre[pl.ds(r0, 64), pl.ds(c0, 256)] = dp.astype(BF16)
                for t in range(taps):
                    r.w_acc[t, :, pl.ds(c0, 256)] += jnp.sum((dp * shifts[t]).reshape(8, 8, 256), axis=0)
                r.w_acc[taps, :, pl.ds(c0, 256)] += jnp.sum(dp.reshape(8, 8, 256), axis=0)

            loop(conv_ch // 256, conv_cols)

        with scope("bo_conv"):
            loop(CHUNK // 64, conv_tile)
        if after is not None:
            after(i, c)

    loop(chunks, chunk)
    for k in range(taps + 1):
        r.small[k : k + 1, :] = jnp.sum(r.w_acc[k], axis=0, keepdims=True)
    d = r.tok.shape[1]
    r.small[6:7, d : d + LANES] = r.bias_acc[...]
    r.small[6:7, d + LANES : d + 2 * LANES] = r.rate_acc[...]


def conv_back(r, c):
    conv_ch = r.raw.shape[1]
    taps = r.conv_w.shape[0]

    def conv_tile(k):
        r0 = aligned(c * CHUNK + k * 64, 64)

        def conv_cols(j):
            c0 = aligned(j * 256, 256)
            window = r.d_pre[pl.ds(r0, 64 + HALO), pl.ds(c0, 256)].astype(F32)
            total = jnp.zeros((64, 256), F32)
            for t in range(taps):
                off = taps - 1 - t
                total = total + r.conv_w[t : t + 1, pl.ds(c0, 256)] * window[off : off + 64]
            r.act[pl.ds(r0, 64), pl.ds(c0, 256)] = total.astype(BF16)

        loop(conv_ch // 256, conv_cols)

    with scope("conv_back"):
        loop(CHUNK // 64, conv_tile)
        rows = chunk_rows(c)
        r.act[rows, conv_ch : conv_ch + LANES] = r.d_dt[rows, :]


def gate_weights(r, rows):
    n = r.normed_t[rows, :]
    ct = 512

    def cols(j):
        at = pl.ds(aligned(j * ct, ct), ct)
        r.gw_gate[rows, at] = dot(n, r.gate[:, at]).astype(r.gw_gate.dtype)

    loop(r.gate.shape[1] // ct, cols)


def rest_weights(r, rows):
    n = r.normed_t[rows, :]
    ct = 512
    inner, width = r.dy.shape[1], r.gw_rest.shape[1]

    def cols(j):
        at = pl.ds(aligned(j * ct, ct), ct)
        r.gw_rest[rows, at] = dot(n, r.act[:, at]).astype(r.gw_rest.dtype)

    loop(inner // ct, cols)
    r.gw_rest[rows, inner:] = dot(n, r.act[:, inner:width]).astype(r.gw_rest.dtype)


def tokens_back(r, c, give=None):
    inner = r.dy.shape[1]
    width = r.w_in.shape[1] - inner
    d = r.tok.shape[1]
    rows = chunk_rows(c)
    with scope("it_dot"):
        r.wide[:, 0:d] = dot(r.gate[rows, :], r.w_in[:, 0:inner], LAST) + dot(r.act[rows, 0:width], r.w_in[:, inner:], LAST)

    def some_rows(j):
        sub = pl.ds(aligned(j * 32, 16), 32)
        at = pl.ds(aligned(c * CHUNK + j * 32, 16), 32)
        t = r.tok[pl.ds(aligned(c * CHUNK + j * 32 + HALO, 16), 32), :].astype(F32)
        scale = lax.rsqrt(jnp.mean(t * t, axis=-1, keepdims=True) + EPSILON)
        unit = t * scale
        g = r.wide[sub, 0:d]
        both = g * unit
        r.in_acc[...] = r.in_acc[...] + (both[0:8] + both[8:16]) + (both[16:24] + both[24:32])
        scaled = g * r.gain_in[...]
        back = scale * (scaled - unit * jnp.mean(unit * scaled, axis=-1, keepdims=True))
        r.grad[at, :] = (r.og[at, :].astype(F32) + back).astype(BF16)

    with scope("it_elem"):
        loop(CHUNK // 32, some_rows)
    if give is not None:
        give(c)


def project_stage(r):
    fill_spread(r.e, LANES // 2)
    r.dt_raw[...] = jnp.zeros_like(r.dt_raw)
    project_block(r, 0, halo=True)
    loop(r.act.shape[0] // CHUNK, lambda c: project_block(r, c), 1)
    conv_act(r)
    scan_states(r)
    project_gate(r)


def mix_stage(r):
    fill_spread(r.e, LANES // 2)
    r.small[...] = jnp.zeros_like(r.small)
    r.gate[...] = r.gate_in[...]
    r.states[...] = r.states_in[...]
    mix_inside(r)
    loop(r.gate.shape[0] // CHUNK, lambda c: out_cotangent(r, c))
    mix_outside(r)
    out_weights(r)


def back_stage(r):
    fill_spread(r.e, LANES // 2)
    r.small[...] = jnp.zeros_like(r.small)
    r.d_pre[r.dy.shape[0] :, :] = jnp.zeros((HALO, r.d_pre.shape[1]), BF16)
    r.y[...] = r.y_in[...]
    r.dxd[...] = r.direct[...]
    back_inside(r)
    r.leaving[...] = r.left[...]
    back_outside(r)


def input_stage(r):
    r.small[...] = jnp.zeros_like(r.small)
    r.in_acc[...] = jnp.zeros_like(r.in_acc)
    chunks = r.dy.shape[0] // CHUNK
    loop(chunks, lambda c: conv_back(r, c))

    def block(i):
        rows = pl.ds(aligned(i * 96, 96), 96)
        gate_weights(r, rows)
        rest_weights(r, rows)

    loop(r.normed_t.shape[0] // 96, block)
    loop(chunks, lambda c: tokens_back(r, c))
    r.small[6:7, 0 : r.tok.shape[1]] = jnp.sum(r.in_acc[...], axis=0, keepdims=True)


def chunk_block(z, size, offset):
    return pl.ds(aligned(z * size + offset, 16), size)


def whole_stage(r):
    p = Place()
    r.leave, r.leaving = r.state, r.enter
    r.small = r.stages.at[0]
    r.dt_bias, r.a_log = r.head_rows.at[0:1, :], r.head_rows.at[1:2, :]
    size = r.block_in.shape[1]
    length, inner = r.dy.shape
    d, proj = r.w_in.shape
    conv_ch = r.raw.shape[1]
    taps = r.conv_w.shape[0]
    chunks = length // CHUNK
    unit = r.w_in_own.shape[0]
    last = 7

    gather = Gather(p, r.w_in_own, r.w_in, slice(inner, proj), r.gather_sems, direct=True)
    gather_gate = Gather(p, r.w_in_own, r.w_in, slice(0, inner), r.gate_sems)
    gather_out = Gather(p, r.w_out_own, r.w_out, slice(0, d), r.out_sems)
    tokens = Exchange(p, lambda z: r.block_in.at[z], lambda z: r.tok.at[chunk_block(z, size, HALO), :], r.tok_sems)
    cotangents = Exchange(p, lambda z: r.out_grad.at[z], lambda z: r.og.at[chunk_block(z, size, 0), :], r.og_sems)
    outputs = Exchange(p, lambda z: r.out.at[chunk_block(z, size, 0), :], lambda z: r.block_out.at[z], r.result_sems)
    grads = Exchange(p, lambda z: r.grad.at[chunk_block(z, size, 0), :], lambda z: r.in_grad.at[z], r.grad_sems)
    forth = Chain(p, r.state, r.decay, r.enter, r.e, True, r.chain_bufs + r.forth_bufs, r.forth_sems)
    back = Chain(p, r.leave, r.decay, r.leaving, r.e, False, r.chain_bufs + r.back_bufs, r.back_sems)
    sum_out = Reduce(p, r.gw_out, r.owned_out, slice(0, d), r.sum_out_bufs, r.sum_out_sems)
    sum_gate = Reduce(p, r.gw_gate, r.owned_in, slice(0, inner), r.sum_gate_bufs, r.sum_gate_sems)
    sum_rest = Reduce(p, r.gw_rest, r.owned_in, slice(inner, proj), r.sum_rest_bufs, r.sum_rest_sems)
    total = Total(p, r.stages, r.small_landed, r.total_sems)

    forth.clear()
    back.clear()
    halo_out = (p.z == 3) & (p.s < last)
    targets = [(p.at(z=(p.z + k) % 4), None) for k in (1, 2, 3)]
    targets += [(p.at(s=s), None) for s in (p.s_core, p.s_x, p.s_y, p.s_diag)]
    targets += [(p.at(s=p.s + 1, z=q), halo_out) for q in range(4)]
    targets += [(p.at(s=p.s - 1, z=3), p.s > 0)]
    targets += [(p.at(s=p.s - 1), p.s > 0), (p.at(s=p.s + 1), p.s < last)]
    with scope("greet"):
        r.d_pre[length:, :] = jnp.zeros((HALO, conv_ch), BF16)
        greet(targets, 7 + jnp.where(p.s > 0, 2, 0) + jnp.where(p.s < last, 1, 0) + jnp.where(halo_out, 4, 0))

    gather.start()
    tokens.keep()
    for k in (1, 2, 3):
        tokens.push_next(k)
    halo = r.tok.at[0:HALO, :]

    @pl.when(halo_out)
    def _():
        for q in range(4):
            send(r.block_in.at[q, size - HALO : size, :], halo, r.halo_send.at[q], r.halo_recv, p.at(s=p.s + 1, z=q))

    r.stages[...] = jnp.zeros_like(r.stages)
    r.dt_raw[...] = jnp.zeros_like(r.dt_raw)
    r.in_acc[...] = jnp.zeros_like(r.in_acc)
    fill_spread(r.e, LANES // 2)
    r.gain_in[...] = r.gain_in_row[...].reshape(1, d)
    r.gain_out[...] = r.gain_out_row[...].reshape(1, inner)
    r.conv_b[...] = r.conv_b_row[...].reshape(1, conv_ch)
    r.skip[...] = spread(jnp.broadcast_to(r.head_rows[2:3, :], (8, LANES)), r.e)[0:1]

    @pl.when(p.s == 0)
    def _():
        r.tok[0:HALO, :] = jnp.zeros((HALO, d), BF16)

    with scope("gather"):
        steps = gather.steps()
        for step in steps[:-1]:
            step()
    gather_gate.start()
    gather_out.start()
    with scope("gather_others"):
        steps[-1]()
    for k in range(4):
        with scope("take_tokens"):
            z = tokens.take(k)
            if k == 3:

                @pl.when(p.s > 0)
                def _():
                    arrived(halo, r.halo_recv)

        with scope("project_block"):
            project_block(r, z, halo=k == 3)

    def both_steps(a, b, extra):
        def run():
            a()
            b()
            if extra is not None:
                extra()

        return run

    def push_cotangents():
        cotangents.keep()
        for k in (1, 2, 3):
            cotangents.push_next(k)

    steps = [
        both_steps(a, b, push_cotangents if i == 5 else None)
        for i, (a, b) in enumerate(zip(gather_gate.steps(), gather_out.steps()))
    ]
    with scope("conv_act"):
        conv_act(r, steps[:8])
    with scope("scan_states"):
        scan_states(r, steps[8:])
    forth.start()
    with scope("project_gate"):
        project_gate(r, [None, forth.chip])
    with scope("mix_inside"):
        mix_inside(r)
    with scope("cotangents"):
        cotangents.finish()
    with scope("out_cotangent"):
        loop(chunks - 1, lambda c: out_cotangent(r, c))
    with scope("enter"):
        forth.enter_chip()
    with scope("out_cotangent"):
        out_cotangent(r, chunks - 1)
    with scope("forth_finish"):
        forth.finish()
    with scope("mix_outside"):
        mix_outside(r, outputs.give)
        forth.drain()
    back.start()
    with scope("out_weights"):
        out_weights(r)
    for k in (3, 1, 2, 0):
        sum_out.cross(k)
    with scope("back_chip"):
        back.chip()
    others = [pl.ds(aligned(p.core_of(s) * 4 * unit, 16), 4 * unit) for s in sum_gate.columns]
    own = [pl.ds(aligned(s * 4 * unit, 16), 4 * unit) for s in sum_gate.columns]
    with scope("gate_weights"):
        for k in (3, 1, 2, 0):
            gate_weights(r, others[k])
            sum_gate.cross(k)
        for k in range(4):
            gate_weights(r, own[k])

    def both_sideways(each):
        def run():
            each.sideways(0)
            each.sideways(1)

        return run

    with scope("back_inside"):
        back_inside(r, [sum_out.diagonal, sum_gate.diagonal, both_sideways(sum_out), None])
    with scope("back_enter"):
        back.enter_chip()
        back.finish()
    front, end = r.d_pre.at[0:HALO, :], r.d_pre.at[length : length + HALO, :]

    def after(i, c):
        with scope("bo_hook"):
            at_step(i, [both_sideways(sum_gate), sum_out.column, sum_gate.column, sum_out.own])

        @pl.when((i == chunks - 1) & (p.s > 0))
        def _():
            send(front, end, r.edge_send, r.edge_recv, p.at(s=p.s - 1))

        @pl.when(i > 0)
        def _():
            conv_back(r, c)
            tokens_back(r, c, grads.give)

    with scope("back_outside"):
        back_outside(r, after)
    with scope("edge"):

        @pl.when(p.s < last)
        def _():
            arrived(end, r.edge_recv)

    conv_back(r, chunks - 1)
    tokens_back(r, chunks - 1, grads.give)
    r.small[6:7, 0:d] = jnp.sum(r.in_acc[...], axis=0, keepdims=True)
    total.push(0)
    with scope("rest_weights"):
        for k in (3, 1, 2, 0):
            rest_weights(r, others[k])
            sum_rest.cross(k)
        total.take(0)
        total.push(1)
        for k in (3, 1, 2, 0):
            rest_weights(r, own[k])
            if k == 3:
                sum_rest.diagonal()
            elif k == 1:
                total.take(1)
                total.push(2)
            elif k == 2:
                total.take(2)
                total.push(3)
    with scope("rest_sideways"):
        sum_rest.sideways(0)
        sum_rest.sideways(1)
    with scope("gate_own"):
        sum_gate.own()
    with scope("rest_column"):
        sum_rest.column()
    with scope("total"):
        total.finish(r.summed)
    r.conv_w_grad[...] = r.summed[0:taps, :]
    r.conv_b_grad[...] = r.summed[taps : taps + 1, :].reshape(conv_ch)
    r.gain_out_grad[...] = r.summed[5:6, 0:inner].reshape(inner)
    r.gain_in_grad[...] = r.summed[6:7, 0:d].reshape(d)
    heads = r.bias_grad.shape[0]
    for k, ref in enumerate((r.bias_grad, r.rate_grad, r.skip_grad)):
        ref[...] = r.summed[6:7, d + k * LANES : d + (k + 1) * LANES][:, 0:heads].reshape(heads)
    with scope("rest_own"):
        sum_rest.own()
    with scope("end"):
        grads.finish()
        outputs.finish()
        for each in (
            gather, gather_gate, gather_out, tokens, cotangents, outputs, grads, back, sum_out, sum_gate, sum_rest, total
        ):
            each.drain()

        @pl.when(halo_out)
        def _():
            for q in range(4):
                arrived(halo, r.halo_send.at[q])

        @pl.when(p.s > 0)
        def _():
            arrived(front, r.edge_send)


def call(stage, name, operands, outs, scratch, in_hbm=(), out_hbm=(), sems={}, collective=None):
    given, made = list(operands), list(outs)
    flat, groups = [], []
    for key, spec in list(scratch.items()) + list(sems.items()):
        many = isinstance(spec, list)
        entries = spec if many else [spec]
        flat += [pltpu.VMEM(*x) if isinstance(x, tuple) else x for x in entries]
        groups.append((key, len(entries), many))

    def kernel(*refs):
        r = Refs(given + made, refs[: len(given) + len(made)])
        rest = list(refs[len(given) + len(made) :])
        for key, count, many in groups:
            part, rest = rest[:count], rest[count:]
            setattr(r, key, part if many else part[0])
        stage(r)

    params = {} if collective is None else {"collective_id": collective, "has_side_effects": True}
    results = pl.pallas_call(
        kernel,
        out_shape=[jax.ShapeDtypeStruct(*outs[k]) for k in made],
        in_specs=[HBM if k in in_hbm else VMEM for k in given],
        out_specs=[HBM if k in out_hbm else VMEM for k in made],
        scratch_shapes=flat,
        compiler_params=pltpu.CompilerParams(vmem_limit_bytes=VMEM_LIMIT, **params),
        name=name,
    )(*operands.values())
    return dict(zip(made, results))


def shards(block_in, gain_in, w_in, conv_w, conv_b, dt_bias, a_log, d_skip, gain_out, w_out, out_grad):
    both = ("shard", "head")
    ranges, groups = lax.axis_size("shard"), lax.axis_size("head")
    head_index = lax.axis_index("head")
    seqs, segment, d = block_in.shape
    inner = gain_out.shape[0]
    heads = dt_bias.shape[0]
    conv_ch = conv_b.shape[0]
    taps = conv_w.shape[0]
    state_n = (conv_ch - inner) // 2
    proj = w_in.shape[1]
    parts = groups // seqs
    length = segment * (groups // parts)
    chunks = length // CHUNK
    ext = length + HALO
    pad = LANES - heads
    shape = dict(
        tok=((ext, d), BF16), og=((length, d), BF16), w_in=((d, proj), BF16), w_out=((inner, d), BF16),
        normed=((ext, d), BF16), normed_t=((d, length), BF16), gate=((length, inner), BF16), raw=((ext, conv_ch), BF16),
        dt_raw=((length, LANES), F32), act=((length, conv_ch + LANES), BF16), dt=((length, LANES), F32),
        cum=((length, LANES), F32), cum_t=((chunks, LANES, CHUNK), F32), states=((chunks + 1, state_n, inner), F32),
        decay=((8, LANES), F32), e=((2 * LANES, inner), BF16), state=((state_n, inner), F32),
        y=((chunks, state_n, inner), F32), xd=((CHUNK, inner), BF16), enter=((state_n, inner), F32),
        wide=((CHUNK, conv_ch), F32), gn=((CHUNK, inner), BF16), gn_t=((inner, length), BF16), acc=((8, inner), F32),
        skip_acc=((1, LANES), F32), out=((length, d), BF16), dy=((length, inner), BF16), y_dot=((length, LANES), F32),
        leave=((state_n, inner), F32), gw_out=((inner, d), BF16), dxd=((chunks, CHUNK, inner), F32),
        d_scores=((chunks, CHUNK, CHUNK), BF16), d_c=((length, state_n), F32), leaving=((state_n, inner), F32),
        w_acc=((taps + 1, 8, conv_ch), F32), bias_acc=((1, LANES), F32), rate_acc=((1, LANES), F32),
        d_pre=((ext, conv_ch), BF16), d_dt=((length, LANES), BF16), gw_gate=((d, inner), BF16),
        gw_rest=((d, proj - inner), BF16), in_acc=((8, d), F32), grad=((length, d), BF16), small=((8, conv_ch), F32),
    )
    assert CHUNK == state_n and segment == CHUNK and 2 * inner // heads == LANES

    def pick(*names):
        return {k: shape[k] for k in names}

    def take(source, *names):
        return {k: source[k] for k in names}

    if (ranges, groups, seqs) == (8, 4, 4):
        head_rows = jnp.pad(jnp.stack([dt_bias, a_log, d_skip]), ((0, 5), (0, pad)))
        made = call(
            whole_stage,
            "block",
            dict(
                block_in=block_in, out_grad=out_grad, w_in_own=w_in, w_out_own=w_out, gain_in_row=gain_in, gain_out_row=gain_out,
                conv_w=conv_w, conv_b_row=conv_b, head_rows=head_rows,
            ),
            dict(
                block_out=(block_in.shape, BF16), in_grad=(block_in.shape, BF16), owned_in=(w_in.shape, F32),
                owned_out=(w_out.shape, F32), gain_in_grad=((d,), F32), conv_w_grad=((taps, conv_ch), F32),
                conv_b_grad=((conv_ch,), F32), bias_grad=((heads,), F32), rate_grad=((heads,), F32), skip_grad=((heads,), F32),
                gain_out_grad=((inner,), F32),
            ),
            {k: v for k, v in shape.items() if k not in ("small", "leave", "leaving")}
            | dict(
                gain_in=((1, d), F32), gain_out=((1, inner), F32), conv_b=((1, conv_ch), F32), skip=((1, inner), F32),
                stages=((4, 8, conv_ch), F32), small_landed=((6, 8, conv_ch), F32), summed=((8, conv_ch), F32),
                chain_bufs=Chain.buffers(state_n, inner)[0], forth_bufs=Chain.buffers(state_n, inner)[1],
                back_bufs=Chain.buffers(state_n, inner)[1], sum_out_bufs=Reduce.buffers(*w_out.shape),
                sum_gate_bufs=Reduce.buffers(w_in.shape[0], inner), sum_rest_bufs=Reduce.buffers(w_in.shape[0], proj - inner),
            ),
            in_hbm=("block_in", "out_grad", "w_in_own", "w_out_own"),
            out_hbm=("block_out", "in_grad"),
            sems=dict(
                gather_sems=Gather.SEMS, gate_sems=Gather.SEMS, out_sems=Gather.SEMS, tok_sems=Exchange.SEMS,
                og_sems=Exchange.SEMS, result_sems=Exchange.SEMS, grad_sems=Exchange.SEMS, forth_sems=Chain.SEMS,
                back_sems=Chain.SEMS, sum_out_sems=Reduce.SEMS, sum_gate_sems=Reduce.SEMS, sum_rest_sems=Reduce.SEMS,
                total_sems=Total.SEMS, halo_send=pltpu.SemaphoreType.DMA((4,)), halo_recv=pltpu.SemaphoreType.DMA,
                edge_send=pltpu.SemaphoreType.DMA, edge_recv=pltpu.SemaphoreType.DMA,
            ),
            collective=0,
        )
        return (
            made["block_out"], made["in_grad"].astype(F32), made["gain_in_grad"], made["owned_in"], made["conv_w_grad"],
            made["conv_b_grad"], made["bias_grad"], made["rate_grad"], made["skip_grad"], made["gain_out_grad"],
            made["owned_out"],
        )

    rows = dict(
        gain_in=gain_in[None], conv_w=conv_w, conv_b=conv_b[None], dt_bias=jnp.pad(dt_bias, (0, pad))[None],
        a_log=jnp.pad(a_log, (0, pad))[None], skip=jnp.repeat(d_skip, inner // heads)[None], gain_out=gain_out[None],
    )
    members = [(s, h) for s in range(ranges) for h in range(groups)]
    index = {m: i for i, m in enumerate(members)}

    def after(s, h):
        return (s, h + 1) if (h + 1) % parts else (s + 1, h + 1 - parts)

    forth = [(index[m], index[after(*m)]) for m in members if after(*m) in index]
    back = [(b, a) for a, b in forth]

    def to_ranges(array):
        if parts == 1:
            return lax.all_to_all(array, "head", split_axis=0, concat_axis=1, tiled=True)[0]
        everything = lax.all_gather(array, "head", axis=1, tiled=True)
        mine = lax.dynamic_index_in_dim(everything, head_index // parts, 0, False)
        return lax.dynamic_slice_in_dim(mine, (head_index % parts) * length, length, 0)

    def to_blocks(array):
        if parts == 1:
            return lax.all_to_all(array[None], "head", split_axis=1, concat_axis=0, tiled=True)
        everything = lax.all_gather(array, "head", axis=0, tiled=True).reshape(seqs, groups * segment, -1)
        return lax.dynamic_slice_in_dim(everything, head_index * segment, segment, 1)

    def chain(own, decay, route):
        def hop(_, before):
            return lax.ppermute((decay * before.astype(F32) + own).astype(BF16), both, route)

        return lax.fori_loop(0, ranges * parts - 1, hop, jnp.zeros(own.shape, BF16)).astype(F32)

    tok, og = to_ranges(block_in), to_ranges(out_grad)
    tok = jnp.concatenate([lax.ppermute(tok[-HALO:], both, forth), tok], axis=0)
    full_in = lax.all_gather(w_in, both, axis=0, tiled=True)
    full_out = lax.all_gather(w_out, both, axis=0, tiled=True)
    v = call(
        project_stage,
        "project",
        dict(tok=tok, w_in=full_in, **take(rows, "gain_in", "conv_w", "conv_b", "dt_bias", "a_log")),
        pick("normed", "normed_t", "gate", "raw", "dt_raw", "act", "dt", "cum", "cum_t", "states", "decay"),
        pick("e", "state"),
    )
    decay = jnp.repeat(jnp.exp(v["decay"][0, :heads]), inner // heads)[None]
    m = call(
        mix_stage,
        "mix",
        dict(
            tok=tok, og=og, w_out=full_out, enter=chain(v["states"][chunks], decay, forth), gate_in=v["gate"],
            states_in=v["states"], **take(v, "act", "dt", "cum", "cum_t"), **take(rows, "gain_out", "skip"),
        ),
        pick("out", "dy", "small", "y", "dxd", "leave", "gate", "states") | dict(gw_out=((inner, d), F32)),
        pick("e", "xd", "gn", "gn_t", "acc"),
    )
    b = call(
        back_stage,
        "back",
        dict(
            tok=tok, left=chain(m["leave"], decay, back), y_in=m["y"], direct=m["dxd"], **take(m, "dy", "states"),
            **take(v, "raw", "dt_raw", "act", "dt", "cum", "cum_t"),
            **take(rows, "conv_w", "conv_b", "dt_bias", "a_log", "skip"),
        ),
        pick("d_pre", "d_dt", "small"),
        pick("e", "xd", "y", "y_dot", "dxd", "d_scores", "d_c", "wide", "w_acc", "bias_acc", "rate_acc", "skip_acc", "leaving"),
    )
    d_pre = b["d_pre"].at[length:].set(lax.ppermute(b["d_pre"][:HALO], both, back))
    i = call(
        input_stage,
        "input",
        dict(
            tok=tok, og=og, w_in=full_in, gate=m["gate"], d_pre=d_pre, d_dt=b["d_dt"], dy=m["dy"], raw=v["raw"],
            normed_t=v["normed_t"], **take(rows, "gain_in", "conv_w"),
        ),
        pick("grad", "small") | dict(gw_gate=((d, inner), F32), gw_rest=((d, proj - inner), F32)),
        pick("act", "wide", "in_acc"),
    )
    gw_in = jnp.concatenate([i["gw_gate"], i["gw_rest"]], axis=1)
    owned_in = lax.psum_scatter(gw_in, both, scatter_dimension=0, tiled=True)
    owned_out = lax.psum_scatter(m["gw_out"], both, scatter_dimension=0, tiled=True)
    small = lax.psum(m["small"] + b["small"] + i["small"], both)
    return (
        to_blocks(m["out"]),
        to_blocks(i["grad"]).astype(F32),
        small[6, :d],
        owned_in,
        small[:taps],
        small[taps],
        small[6, d : d + heads],
        small[6, d + LANES : d + LANES + heads],
        small[6, d + 2 * LANES : d + 2 * LANES + heads],
        small[5, :inner],
        owned_out,
    )


def solution(mesh):
    rows, tokens = P(("shard", "head"), None), P(None, ("shard", "head"), None)
    return jax.shard_map(
        shards,
        mesh=mesh,
        in_specs=(tokens, P(), rows, P(), P(), P(), P(), P(), P(), rows, tokens),
        out_specs=(tokens, tokens, P(), rows, P(), P(), P(), P(), P(), P(), rows),
        check_vma=False,
    )
```
